32 devices in a mesh: band: 8 (over z, x), grid: 4 (over y, core).
Axes of the slice: x: 2, y: 2, z: 4, core: 2. Of those that a mesh axis runs over, the one named last changes fastest.
Arguments:
- partial_density: float32 [8, 128, 128, 128], P('band', 'grid'), may hold values from 0.01 to 1
- node_index: int32 [128, 128, 128], P('grid'), may hold values from 0 to 19
- node_weight: float32 [4, 128, 128, 128], P(None, 'grid'), may hold values from 0 to 1
- node_slope: float32 [4, 128, 128, 128], P(None, 'grid'), may hold values from -6 to 6
- kernel_table: float32 [20, 20, 114], replicated, may hold values from -0.8 to 0.8, as said below
Outputs:
- potential: float32 [128, 128, 128], P('grid')
The draws below stay inside these ranges and needn't reach their ends.
Inputs may be any that keep to these rules, and one draw needn't show every extreme that they name: node_index(r) is the node at the lower end of the interval of q0 at r; nodes node_index - 1 to node_index + 2 carry the four weights. `kernel_table`: symmetric in its first two indices.
All inputs are finite; a program needn't handle non-finite values.
Results may differ from the reference program's by a relative error of at most 0.0003.
Values sent between devices are 32-bit elements; how exact they have to be, the bound alone decides.
A program may use at most 128 MiB of HBM per device.

```python
import math
import jax
import jax.numpy as jnp
from jax import lax

N = 128
NA = 20
SHELLS = 114
GROUPS = 8


def draw_kernel_table(key, part):
    sample_values = jax.random.truncated_normal(key, -4.0, 4.0, (NA, NA, SHELLS), jnp.float32) * 0.2
    symmetric = 0.5 * (sample_values + jnp.transpose(sample_values, (1, 0, 2)))
    return symmetric


def touch_ends(array, own_key, least, largest):
    place = [jax.random.randint(jax.random.fold_in(own_key, axis), (), 0, length) for axis, length in enumerate(array.shape)]
    widest = array.shape.index(max(array.shape))
    next_to = place[:widest] + [(place[widest] + 1) % array.shape[widest]] + place[widest + 1:]
    return array.at[tuple(place)].set(least).at[tuple(next_to)].set(largest)


def block_scale(own_key, extent, split, smallest, high):
    level = 1.0
    for position, parts in split:
        steps = jax.random.uniform(jax.random.fold_in(jax.random.fold_in(own_key, 6), position), (parts,), jnp.float32, smallest / len(split), high / len(split))
        level = level * jnp.repeat(jnp.exp(steps), extent[position] // parts).reshape((-1,) + (1,) * (len(extent) - 1 - position))
    return level


def noise(key, shape, width, reach, pieces=(), kind=jnp.bfloat16):
    drawn = width * jax.random.normal(key, shape, jnp.float32)
    if pieces:
        drawn = drawn * block_scale(key, shape, pieces, -0.22, 0.18)
    return jnp.clip(drawn, -reach, reach).astype(kind)


def setup_inputs(seed: int = 0) -> dict:
    seeds = jax.random.split(jax.random.key(seed), 6)
    partial_density = jnp.clip(jnp.exp(math.log(1.0) - 4.6051702 * jax.random.uniform(seeds[0], (GROUPS, N, N, N), jnp.float32) ** block_scale(seeds[0], (GROUPS, N, N, N), ((0, 8), (1, 4)), -0.2, 0.2)), 0.01, 1.0)
    node_index = touch_ends(jax.random.randint(seeds[1], (N, N, N), 0, NA), jax.random.fold_in(seeds[1], 1), 0, NA - 1).astype(jnp.int32)
    node_weight = jnp.clip(1.0 * jax.random.uniform(seeds[2], (4, N, N, N), jnp.float32) ** block_scale(seeds[2], (4, N, N, N), ((1, 4),), -0.2, 0.2), 0.0, 1.0)
    node_slope = noise(seeds[3], (4, N, N, N), 1.0, 6.0, ((1, 4),), jnp.float32)
    kernel_table = draw_kernel_table(jax.random.fold_in(seeds[5], 71), 0)
    return {"partial_density": partial_density, "node_index": node_index, "node_weight": node_weight, "node_slope": node_slope, "kernel_table": kernel_table}


def frequency(length):
    positions = jnp.arange(length, dtype=jnp.int32)
    return jnp.where(positions < length // 2, positions, positions - length)

def shell_split(square_norm):
    root_value = jnp.sqrt(square_norm.astype(jnp.float32))
    shell_idx = root_value.astype(jnp.int32)
    shell_idx = shell_idx - (shell_idx * shell_idx > square_norm).astype(jnp.int32)
    shell_idx = shell_idx + ((shell_idx + 1) * (shell_idx + 1) <= square_norm).astype(jnp.int32)
    fraction = root_value - shell_idx.astype(jnp.float32)
    return (shell_idx, fraction)

def node_fields(count_nodes, intervals, weights):
    node_ids = jnp.arange(count_nodes, dtype=jnp.int32)
    summed = jnp.zeros((count_nodes,) + intervals.shape, jnp.float32)
    for offset in range(4):
        matched = node_ids[:, None, None, None] == (intervals + (offset - 1))[None]
        summed = summed + jnp.where(matched, weights[offset][None], jnp.zeros((), jnp.float32))
    return summed

def reference(partial_density, node_index, node_weight, node_slope, kernel_table):
    density = lax.optimization_barrier(jnp.sum(partial_density, axis=0))
    theta_fields = density[None] * node_fields(NA, node_index, node_weight)
    spectrum = jnp.fft.fftn(theta_fields, axes=(1, 2, 3))
    spec_real = jnp.real(spectrum)
    spec_imag = jnp.imag(spectrum)
    freq_all = frequency(N)
    plane_norm = freq_all[:, None] * freq_all[:, None] + freq_all[None, :] * freq_all[None, :]

    def mix_plane(plane_idx):
        freq_x = freq_all[plane_idx]
        shell_idx, fraction = shell_split(plane_norm + freq_x * freq_x)
        lower_values = kernel_table[:, :, shell_idx]
        upper_values = kernel_table[:, :, shell_idx + 1]
        kernel = (1.0 - fraction) * lower_values + fraction * upper_values
        plane_real = lax.dynamic_index_in_dim(spec_real, plane_idx, 1, keepdims=False)
        plane_imag = lax.dynamic_index_in_dim(spec_imag, plane_idx, 1, keepdims=False)
        out_real = jnp.einsum('abyz,ayz->byz', kernel, plane_real, precision=lax.Precision.HIGHEST)
        out_imag = jnp.einsum('abyz,ayz->byz', kernel, plane_imag, precision=lax.Precision.HIGHEST)
        return (out_real, out_imag)
    mixed_real, mixed_imag = lax.map(mix_plane, jnp.arange(N, dtype=jnp.int32))
    mixed = jnp.moveaxis(mixed_real + 1j * mixed_imag, 0, 1)
    fields = jnp.real(jnp.fft.ifftn(mixed, axes=(1, 2, 3)))
    return lax.optimization_barrier(jnp.sum(fields * node_fields(NA, node_index, node_slope), axis=0))
```

```python
import math

import jax
import jax.numpy as jnp
import numpy as np
from jax import lax
from jax.experimental import pallas as pl
from jax.experimental.pallas import tpu as pltpu
from jax.sharding import PartitionSpec as P

def frequency_of(positions, length):
    return jnp.where(positions < length // 2, positions, positions - length)


def shell_split(square_norm):
    root_value = jnp.sqrt(square_norm.astype(jnp.float32))
    shell_idx = root_value.astype(jnp.int32)
    shell_idx = shell_idx - (shell_idx * shell_idx > square_norm).astype(jnp.int32)
    shell_idx = shell_idx + ((shell_idx + 1) * (shell_idx + 1) <= square_norm).astype(jnp.int32)
    fraction = root_value - shell_idx.astype(jnp.float32)
    return (shell_idx, fraction)


def node_fields(count_nodes, intervals, weights):
    node_ids = jnp.arange(count_nodes, dtype=jnp.int32)
    summed = jnp.zeros((count_nodes,) + intervals.shape, jnp.float32)
    for offset in range(4):
        matched = node_ids[:, None, None, None] == (intervals + (offset - 1))[None]
        summed = summed + jnp.where(matched, weights[offset][None], jnp.zeros((), jnp.float32))
    return summed


def phase_table(source_idx, target_idx, modulus):
    product_mod = source_idx[:, None] * target_idx[None, :] % modulus
    angles = product_mod.astype(jnp.float32) * (2.0 * math.pi / modulus)
    return (jnp.cos(angles), jnp.sin(angles))


def contract(pattern, operand, matrix):
    return jnp.einsum(pattern, operand, matrix, precision=lax.Precision.HIGHEST)


def mirrored(values, dim):
    return jnp.roll(jnp.flip(values, dim), 1, dim)


def forward_tables(positions, plane_ids, length):
    cosine, sine = phase_table(positions, plane_ids, length)
    alternating = jnp.where(positions % 2 == 0, 1.0, -1.0).astype(jnp.float32)
    sine = jnp.where(plane_ids[None, :] == 0, -alternating[:, None], sine)
    return (cosine, sine)


def shell_weights_of(square_norm, shell_count):
    shell_ids = jnp.arange(shell_count, dtype=jnp.int32)
    shell_idx, fraction = shell_split(square_norm)
    expand = (slice(None),) + (None,) * square_norm.ndim
    lower_hit = shell_ids[expand] == shell_idx[None]
    upper_hit = shell_ids[expand] == shell_idx[None] + 1
    return jnp.where(lower_hit, 1.0 - fraction[None], 0.0) + jnp.where(
        upper_hit, fraction[None], 0.0
    )


def short(pattern, left, right):
    return jnp.einsum(pattern, left, right, precision=lax.Precision.HIGH)


def halves(values):
    high = values.astype(jnp.bfloat16)
    low = (values - high.astype(jnp.float32)).astype(jnp.bfloat16)
    return high, low


def mix_kernel(count, padded, shell_ref, frac_ref, table_ref, spec_ref, out_ref):
    rows, lanes = shell_ref.shape[1:]
    ids = lax.broadcasted_iota(jnp.int32, (table_ref.shape[1] // 3, lanes), 0)

    def hats(row):
        shell = shell_ref[0, pl.ds(row, 1), :]
        frac = frac_ref[0, pl.ds(row, 1), :]
        return jnp.where(ids == shell, 1.0 - frac, jnp.where(ids == shell + 1, frac, 0.0))

    def step(pair, carry):
        both = jnp.concatenate([hats(2 * pair), hats(2 * pair + 1)], axis=1)
        high, low = halves(both)
        phi = jnp.dot(
            table_ref[...],
            jnp.concatenate([high, high, low], axis=0),
            preferred_element_type=jnp.float32,
        )
        for side in range(2):
            row = 2 * pair + side
            real = jnp.zeros((padded, lanes), jnp.float32)
            imag = jnp.zeros((padded, lanes), jnp.float32)
            for node in range(count):
                part = phi[node * padded : (node + 1) * padded, side * lanes : (side + 1) * lanes]
                real = real + part * spec_ref[0, node, 0, pl.ds(row, 1), :]
                imag = imag + part * spec_ref[1, node, 0, pl.ds(row, 1), :]
            out_ref[0, row, 0] = real[:count]
            out_ref[0, row, 1] = imag[:count]
        return carry

    lax.fori_loop(0, rows // 2, step, 0)


def mix(spectrum, shell, frac, kernel_table):
    _, count, planes, rows, lanes = spectrum.shape
    padded = -(-count // 8) * 8
    depth = -(-(kernel_table.shape[2]) // 128) * 128
    table = jnp.pad(kernel_table, ((0, 0), (0, padded - count), (0, depth - kernel_table.shape[2])))
    table = table.reshape(count * padded, depth)
    rounded = lax.reduce_precision(table, exponent_bits=8, mantissa_bits=7)
    high, low = rounded.astype(jnp.bfloat16), (table - rounded).astype(jnp.bfloat16)
    table = jnp.concatenate([high, low, high], axis=1)
    return pl.pallas_call(
        lambda *refs: mix_kernel(count, padded, *refs),
        grid=(planes,),
        in_specs=[
            pl.BlockSpec((1, rows, lanes), lambda p: (p, 0, 0)),
            pl.BlockSpec((1, rows, lanes), lambda p: (p, 0, 0)),
            pl.BlockSpec(table.shape, lambda p: (0, 0)),
            pl.BlockSpec((2, count, 1, rows, lanes), lambda p: (0, 0, p, 0, 0)),
        ],
        out_specs=pl.BlockSpec((1, rows, 2, count, lanes), lambda p: (p, 0, 0, 0, 0)),
        out_shape=jax.ShapeDtypeStruct((planes, rows, 2, count, lanes), jnp.float32),
    )(shell, frac, table, spectrum)


def per_device(partial_density, node_index, node_weight, node_slope, kernel_table):
    length = node_index.shape[1]
    half = length // 2
    count_nodes = kernel_table.shape[0]
    shell_count = kernel_table.shape[2]
    planes = half // lax.axis_size("band")
    grid_size = lax.axis_size("grid")
    grid_part = length // grid_size
    band_at = lax.axis_index("band")
    grid_at = lax.axis_index("grid")
    full_range = jnp.arange(length, dtype=jnp.int32)
    own_planes = band_at * planes + jnp.arange(planes, dtype=jnp.int32)
    own_rows = grid_at * grid_part + jnp.arange(grid_part, dtype=jnp.int32)
    lower = ((full_range >= 1) & (full_range < half)).astype(jnp.float32)
    upper = (full_range > half).astype(jnp.float32)
    single = 1.0 - lower - upper
    joint = (own_planes == 0)[:, None, None, None, None]
    cosine, sine = phase_table(full_range, full_range, length)
    forward = jnp.stack(
        [jnp.stack([cosine, -sine], 1), jnp.stack([sine, cosine], 1)]
    )
    low_only = lower + single
    packed = jnp.stack(
        [
            jnp.stack([cosine * low_only, -sine * lower], 1),
            jnp.stack([cosine * upper, -sine * upper + cosine * single], 1),
        ]
    )
    forward_y = jnp.where(joint, packed[None], forward[None])
    backward = jnp.stack(
        [jnp.stack([cosine, sine], 1), jnp.stack([-sine, cosine], 1)]
    )
    lower_col, upper_col, single_col = (v[:, None] for v in (lower, upper, single))
    opened = jnp.stack(
        [
            jnp.stack([cosine * (2.0 * lower_col + single_col), cosine * (2.0 * upper_col)], 1),
            jnp.stack(
                [sine * (-2.0 * lower_col), sine * (-2.0 * upper_col) + cosine * single_col], 1
            ),
        ]
    )
    backward_y = jnp.where(joint, opened[None], backward[None])

    density = lax.psum(partial_density[0], "band")
    theta_fields = density[None] * node_fields(count_nodes, node_index, node_weight)
    cosine_z, sine_z = forward_tables(full_range, own_planes, length)
    table_z = jnp.stack([cosine_z, -sine_z], 1)
    columns = short("zcp,axyz->cpaxy", table_z, theta_fields)
    waves = short("cpaxy,pcydw->wdapx", columns, forward_y)
    waves = waves.reshape((grid_size, grid_part) + waves.shape[1:])
    pencils = lax.all_to_all(waves, "grid", split_axis=0, concat_axis=0, tiled=True)
    forward_x = forward.reshape((2, grid_size, grid_part) + forward.shape[2:])
    spectrum = short("gwdapx,dgxev->eapwv", pencils, forward_x)

    freq_x = frequency_of(full_range, length)
    square_x = freq_x * freq_x
    freq_rows = frequency_of(own_rows, length)
    square_rows = freq_rows * freq_rows
    third_square = jnp.where(
        (own_planes[:, None] == 0) & (own_rows[None, :] > half),
        half * half,
        (own_planes * own_planes)[:, None],
    )
    square_norm = (third_square + square_rows[None, :])[:, :, None] + square_x
    shell, frac = shell_split(square_norm)
    mixed = mix(spectrum, shell, frac, kernel_table)

    flag = ((own_rows[0] == 0) | (own_rows[0] == half)) & (own_planes[0] == 0)
    first_norm = square_x + square_rows[0]
    pair_norm = jnp.stack([first_norm, first_norm + half * half])
    kernels = contract("abs,sqx->qabx", kernel_table, shell_weights_of(pair_norm, shell_count))
    spread = (0.5 * flag.astype(jnp.float32)) * (kernels[0] - kernels[1])
    base = spectrum[:, :, 0, 0, :]
    turned = mirrored(base, 2)
    delta = jnp.stack([turned[0] - base[0], -turned[1] - base[1]])
    extra = jnp.sum(spread[None] * delta[:, :, None, :], axis=1)
    mixed = mixed.at[0, 0].add(extra)

    backward_x = backward.reshape(2, length, 2, grid_size, grid_part)
    inverse = short("pwdbv,dvegx->gwebpx", mixed, backward_x)
    returned = lax.all_to_all(inverse, "grid", split_axis=0, concat_axis=0, tiled=True)
    backward_y = backward_y.reshape((planes, 2, grid_size, grid_part, 2, length))
    slab = short("gwdbpx,pdgwcy->cpbxy", returned, backward_y)
    cosine_own, sine_own = phase_table(own_planes, full_range, length)
    alternating = jnp.where(full_range % 2 == 0, 1.0, -1.0).astype(jnp.float32)
    cosine_back = jnp.where(own_planes[:, None] == 0, 1.0, 2.0 * cosine_own)
    sine_back = jnp.where(own_planes[:, None] == 0, -alternating[None, :], 2.0 * sine_own)
    table_back = jnp.stack([cosine_back, -sine_back]) * (1.0 / float(length) ** 3)
    field_parts = short("cpbxy,cpz->bxyz", slab, table_back)
    slopes = node_fields(count_nodes, node_index, node_slope)
    partial_potential = jnp.sum(field_parts * slopes, axis=0)
    return lax.psum(partial_potential, "band")


LANES = 128
SUBLANES = 8
MESH = pl.DeviceIdType.MESH
VMEM = pltpu.VMEM


def split_table(table):
    high = np.asarray(table).astype(jnp.bfloat16)
    low = (np.asarray(table) - high.astype(np.float64)).astype(jnp.bfloat16)
    return high, low


def angles_of(sources, targets, length):
    phase = (np.outer(sources, targets) % length) * (2.0 * np.pi / length)
    return np.cos(phase), np.sin(phase)


def complex_table(cosine, sine):
    return np.stack([np.stack([cosine, -sine], 1), np.stack([sine, cosine], 1)])


def constant_tables(length, bands, planes):
    points = np.arange(length)
    half = length // 2
    cosine, sine = angles_of(points, points, length)
    lower = ((points >= 1) & (points < half)).astype(np.float64)
    upper = (points > half).astype(np.float64)
    single = 1.0 - lower - upper
    forward = complex_table(cosine, sine)
    backward = complex_table(cosine, -sine)
    packed = np.stack(
        [
            np.stack([cosine * (lower + single), -sine * lower], 1),
            np.stack([cosine * upper, -sine * upper + cosine * single], 1),
        ]
    )
    lo, up, one = (v[:, None] for v in (lower, upper, single))
    opened = np.stack(
        [
            np.stack([cosine * (2 * lo + one), cosine * (2 * up)], 1),
            np.stack([sine * (-2 * lo), sine * (-2 * up) + cosine * one], 1),
        ]
    )
    square = (2 * length, 2 * length)

    def right(table):
        high, low = split_table(table.reshape(square))
        return np.concatenate([high, high, low], 0)

    def left(table):
        high, low = split_table(table.reshape(square).T)
        return np.concatenate([high, low, high], 1)

    alternating = np.where(points % 2 == 0, 1.0, -1.0)
    z_forward, z_backward = [], []
    for band in range(bands):
        ids = band * planes + np.arange(planes)
        cos_z, sin_z = angles_of(ids, points, length)
        minus = np.where(ids[:, None] == 0, alternating[None], -sin_z)
        rows = np.concatenate([cos_z, minus], 0)
        high, low = split_table(rows)
        top = np.concatenate([high, high], 1)
        bottom = np.concatenate([low, np.zeros_like(low)], 1)
        z_forward.append(np.concatenate([top, bottom], 0))
        first = ids[:, None] == 0
        rows = np.concatenate(
            [np.where(first, 1.0, 2.0 * cos_z), np.where(first, alternating[None], -2.0 * sin_z)]
        ) / float(length) ** 3
        high, low = split_table(rows.T)
        z_backward.append(np.concatenate([high, low, high], 1))
    return {
        "y_forward": np.stack([right(packed), right(forward)]),
        "y_backward": np.stack([right(opened), right(backward)]),
        "x_forward": left(forward),
        "x_backward": left(backward),
        "z_forward": np.stack(z_forward),
        "z_backward": np.stack(z_backward),
    }


def triple_left(values):
    high, low = halves(values)
    return jnp.concatenate([high, low, high], axis=1)


def triple_right(values):
    high, low = halves(values)
    return jnp.concatenate([high, high, low], axis=0)


def matmul(left, right):
    return jnp.dot(left, right, preferred_element_type=jnp.float32)


def matmul_nt(left, right):
    return lax.dot_general(
        left, right, (((1,), (1,)), ((), ())), preferred_element_type=jnp.float32
    )


def matmul_tn(left, right):
    return lax.dot_general(
        left, right, (((0,), (0,)), ((), ())), preferred_element_type=jnp.float32
    )


def greet(axis, targets):
    barrier = pltpu.get_barrier_semaphore()
    for target in targets:
        pl.semaphore_signal(barrier, inc=1, device_id={axis: target}, device_id_type=MESH)
    pl.semaphore_wait(barrier, len(targets))


def sum_kernel(outer, in_ref, out_ref, near_buf, stage, far_buf, sems):
    me = lax.axis_index("band")
    far, near = me // 2, lax.rem(me, 2)
    partner = far * 2 + (1 - near)
    others = [lax.rem(far + 1 + j, outer) for j in range(outer)]
    back = [lax.rem(far + outer - 1 - j, outer) for j in range(outer)]
    rows = in_ref.shape[0] // 2
    part = rows // outer
    greet("band", [partner] + [o * 2 + near for o in others[:-1]])

    def piece(side, quarter):
        return pl.ds(side * rows + quarter * part, part)

    def remote(src, dst, row, j, target):
        return pltpu.make_async_remote_copy(
            src_ref=src,
            dst_ref=dst,
            send_sem=sems.at[row, 0, j],
            recv_sem=sems.at[row, 1, j],
            device_id={"band": target},
            device_id_type=MESH,
        )

    near_copies = [
        remote(in_ref.at[piece(1 - near, others[j])], near_buf.at[j], 0, j, partner)
        for j in range(outer)
    ]
    for copy in near_copies:
        copy.start()
    far_copies = []
    for j in range(outer - 1):
        near_copies[j].wait_recv()
        stage[j] = in_ref[piece(near, others[j])] + near_buf[j]
        copy = remote(stage.at[j], far_buf.at[j], 1, j, others[j] * 2 + near)
        copy.start()
        far_copies.append(copy)
    near_copies[outer - 1].wait_recv()
    total = in_ref[piece(near, far)] + near_buf[outer - 1]
    for copy in far_copies:
        copy.wait_recv()
    for j in range(outer - 1):
        total = total + far_buf[j]
    own = piece(near, far)
    out_ref[own] = total
    gathers = []
    for j in range(outer - 1):
        copy = remote(out_ref.at[own], out_ref.at[own], 2, j, others[j] * 2 + near)
        copy.start()
        gathers.append(copy)
    passes = [remote(out_ref.at[own], out_ref.at[own], 3, outer - 1, partner)]
    passes[0].start()
    for j in range(outer - 1):
        gathers[j].wait_recv()
        block = out_ref.at[piece(near, back[j])]
        copy = remote(block, block, 3, j, partner)
        copy.start()
        passes.append(copy)
    for copy in passes:
        copy.wait_recv()
    for copy in near_copies + far_copies + gathers + passes:
        copy.wait_send()


def band_sum(values, collective_id):
    outer = lax.axis_size("band") // 2
    part = values.shape[0] // (2 * outer)
    piece = (part,) + values.shape[1:]
    return pl.pallas_call(
        lambda *refs: sum_kernel(outer, *refs),
        in_specs=[pl.BlockSpec(memory_space=VMEM)],
        out_specs=pl.BlockSpec(memory_space=VMEM),
        out_shape=jax.ShapeDtypeStruct(values.shape, jnp.float32),
        scratch_shapes=[
            VMEM((outer,) + piece, jnp.float32),
            VMEM((outer - 1,) + piece, jnp.float32),
            VMEM((outer - 1,) + piece, jnp.float32),
            pltpu.SemaphoreType.DMA((4, 2, outer)),
        ],
        compiler_params=pltpu.CompilerParams(
            collective_id=collective_id, has_side_effects=True, vmem_limit_bytes=60 * 2**20
        ),
    )(values)


def forward_kernel(
    sizes, density_ref, index_ref, weight_ref, tz_ref, ty_ref, out_ref, theta, columns, send, sems
):
    count, grid_size, steps, planes, length = sizes
    step_rows = SUBLANES * length
    band_at, me = lax.axis_index("band"), lax.axis_index("grid")
    order = [lax.rem(me + 1 + j, grid_size) for j in range(grid_size)]
    per = planes // grid_size
    rows = count * SUBLANES
    greet("grid", order[:-1])

    def copy_of(step, slot, j):
        return pltpu.make_async_remote_copy(
            src_ref=send.at[slot, j],
            dst_ref=out_ref.at[:, :, me * steps + step],
            send_sem=sems.at[0, step, j],
            recv_sem=sems.at[1, step, j],
            device_id={"grid": order[j]},
            device_id_type=MESH,
        )

    def fill(step):
        block = 32

        def body(at, carry):
            x_at = step * SUBLANES + at // (length // block)
            start = pl.multiple_of(lax.rem(at, length // block) * block, block)
            place = pl.ds(pl.multiple_of(at * block, block), block)
            index = index_ref[x_at, pl.ds(start, block), :] - 1
            amount = density_ref[x_at, pl.ds(start, block), :]
            parts = [amount * weight_ref[j, x_at, pl.ds(start, block), :] for j in range(4)]
            for node in range(count):
                value = jnp.where(index == node, parts[0], 0.0)
                for j in range(1, 4):
                    value = jnp.where(index == node - j, parts[j], value)
                high, low = halves(value)
                theta[node, place, 0:length] = high
                theta[node, place, length : 2 * length] = low
            return carry

        lax.fori_loop(0, step_rows // block, body, 0)

    def columns_of(step):
        table = tz_ref[band_at]

        def body(node, carry):
            for pair in range(SUBLANES // 2):
                block = theta[node, pair * 2 * length : (pair + 1) * 2 * length, :]
                out = matmul_nt(table, block)
                out = out[: 2 * planes] + out[2 * planes :]
                for side in range(2):
                    for c in range(2):
                        row = c * planes * rows + node * SUBLANES + pair * 2 + side
                        columns[pl.ds(row, planes, stride=rows), :] = out[
                            c * planes : (c + 1) * planes, side * length : (side + 1) * length
                        ]
            return carry

        lax.fori_loop(0, count, body, 0)

    def waves_of(step, slot, j):
        for k in range(per):
            plane = order[j] * per + k
            start = pl.multiple_of(plane * rows, rows)
            left = jnp.concatenate(
                [columns[pl.ds(c * planes * rows + start, rows), :] for c in range(2)], axis=1
            )
            kind = jnp.minimum(plane + band_at * planes, 1)
            out = matmul(triple_left(left), ty_ref[kind])
            for d in range(2):
                value = out[:, d * length : (d + 1) * length]
                if j < grid_size - 1:
                    send[slot, j, k, d] = value
                else:
                    out_ref[k, d, me * steps + step] = value

    for step in range(steps):
        slot = step % 2
        fill(step)
        columns_of(step)
        for j in range(grid_size):
            if step >= 2 and j < grid_size - 1:
                copy_of(step - 2, slot, j).wait_send()
            waves_of(step, slot, j)
            if j < grid_size - 1:
                copy_of(step, slot, j).start()
    for step in range(steps):
        for j in range(grid_size - 1):
            if step >= steps - 2:
                copy_of(step, step % 2, j).wait_send()
            copy_of(step, step % 2, j).wait_recv()


def forward(density, node_index, node_weight, tables, count, planes, grid_size):
    grid_part, length = density.shape[:2]
    steps = grid_part // SUBLANES
    per = planes // grid_size
    sizes = (count, grid_size, steps, planes, length)
    rows = count * SUBLANES
    return pl.pallas_call(
        lambda *refs: forward_kernel(sizes, *refs),
        in_specs=[pl.BlockSpec(memory_space=VMEM)] * 5,
        out_specs=pl.BlockSpec(memory_space=VMEM),
        out_shape=jax.ShapeDtypeStruct(
            (per, 2, grid_size * steps, rows, length), jnp.float32
        ),
        scratch_shapes=[
            VMEM((count, SUBLANES * length, 2 * length), jnp.bfloat16),
            VMEM((2 * planes * rows, length), jnp.float32),
            VMEM((2, grid_size - 1, per, 2, rows, length), jnp.float32),
            pltpu.SemaphoreType.DMA((2, steps, grid_size - 1)),
        ],
        compiler_params=pltpu.CompilerParams(
            collective_id=1, has_side_effects=True, vmem_limit_bytes=60 * 2**20
        ),
    )(density, node_index, node_weight, tables["z_forward"], tables["y_forward"])


def middle_kernel(
    sizes,
    waves_ref,
    shell_ref,
    frac_ref,
    pair_shell_ref,
    pair_frac_ref,
    table_ref,
    tx_ref,
    ti_ref,
    out_ref,
    spec,
    mixed,
    phi,
    extra,
    send,
    sems,
):
    count, padded, grid_size, planes, length, group = sizes
    per = planes // grid_size
    grid_part = length // grid_size
    wide = per * length
    half = length // 2
    band_at, me = lax.axis_index("band"), lax.axis_index("grid")
    order = [lax.rem(me + 1 + j, grid_size) for j in range(grid_size)]
    joint = (band_at == 0) & (me == 0)
    greet("grid", order[:-1])

    lane = lax.broadcasted_iota(jnp.int32, (16, wide), 1)
    slot = lax.broadcasted_iota(jnp.int32, (16, wide), 0)
    chosen = jnp.where(lane == slot * half, 1.0, 0.0)
    chosen = jnp.where(slot < 2, chosen, 0.0).astype(jnp.bfloat16)

    def block_of(node, d):
        parts = [
            waves_ref[k, d, :, pl.ds(pl.multiple_of(node * SUBLANES, SUBLANES), SUBLANES), :]
            for k in range(per)
        ]
        return jnp.concatenate([p.reshape(length, length) for p in parts], axis=1)

    def to_spectrum(node, carry):
        values = jnp.concatenate([block_of(node, 0), block_of(node, 1)], axis=0)
        spec[node] = matmul(tx_ref[...], triple_right(values))
        return carry

    lax.fori_loop(0, count, to_spectrum, 0)

    ids = lax.broadcasted_iota(jnp.int32, (table_ref.shape[1] // 3, wide), 0)

    def hats(shell, frac):
        return jnp.where(ids == shell, 1.0 - frac, jnp.where(ids == shell + 1, frac, 0.0))

    def mix_rows(row_sets, load):
        sums = [jnp.zeros((padded, wide), jnp.float32) for _ in range(2 * len(row_sets))]
        for node in range(count):
            part = phi[node * padded : (node + 1) * padded, :]
            for at, row in enumerate(row_sets):
                for e in range(2):
                    sums[2 * at + e] = sums[2 * at + e] + part * load(node, e, row)
        return sums

    def step(i, carry):
        weights = hats(shell_ref[pl.ds(i, 1), :], frac_ref[pl.ds(i, 1), :])
        phi[...] = matmul(table_ref[...], triple_right(weights))
        rows = [i, lax.rem(length - i, length)]
        sums = mix_rows(rows, lambda node, e, row: spec[node, pl.ds(e * length + row, 1), :])
        for at, row in enumerate(rows):
            for e in range(2):
                start = pl.multiple_of((e * length + row) * padded, SUBLANES)
                for k in range(per):
                    value = sums[2 * at + e][:, k * length : (k + 1) * length]
                    mixed[k, pl.ds(start, padded), :] = value
        return carry

    lax.fori_loop(0, half + 1, step, 0)

    extra[...] = jnp.zeros_like(extra)

    @pl.when(joint)
    def _():
        right = jnp.concatenate(
            [tx_ref[:, length : 2 * length], tx_ref[:, 3 * length : 4 * length]], axis=1
        )

        def gather(node, carry):
            high, low = halves(block_of(node, 1))
            imag = (matmul_nt(chosen, high) + matmul_nt(chosen, low))[:SUBLANES]
            high, low = halves(-2.0 * imag)
            zero = jnp.zeros_like(low)
            left = jnp.concatenate(
                [jnp.concatenate([high, high], 1), jnp.concatenate([low, zero], 1)], axis=0
            )
            delta = matmul_nt(left, right)
            delta = delta[:SUBLANES] + delta[SUBLANES:]
            spec[node, 0:SUBLANES, :] = delta
            return carry

        lax.fori_loop(0, count, gather, 0)
        weights = 0.5 * (
            hats(pair_shell_ref[0:1, :], pair_frac_ref[0:1, :])
            - hats(pair_shell_ref[1:2, :], pair_frac_ref[1:2, :])
        )
        phi[...] = matmul(table_ref[...], triple_right(weights))

        def load(node, e, row):
            return jnp.concatenate(
                [spec[node, r : r + 1, e * length : (e + 1) * length] for r in range(2)], axis=1
            )

        real, imag = mix_rows([0], load)
        for r in range(2):
            left = jnp.concatenate(
                [real[:, r * length : (r + 1) * length], imag[:, r * length : (r + 1) * length]],
                axis=1,
            )
            added = matmul_nt(triple_left(left), right_triple(ti_ref))
            for c in range(2):
                value = added[:, c * length : (c + 1) * length]
                extra[c, pl.ds(r, padded, stride=SUBLANES), :] = value

    def to_slabs(node, carry):
        rows = [mixed[k, pl.ds(node, 2 * length, stride=padded), :] for k in range(per)]
        out = matmul(ti_ref[...], triple_right(jnp.concatenate(rows, axis=1)))
        place = pl.ds(pl.multiple_of(node * SUBLANES, SUBLANES), SUBLANES)
        high, low = halves(jnp.concatenate([extra[c, place, :] for c in range(2)], axis=1))
        both = jnp.concatenate([high, low], axis=0)
        mask = jnp.concatenate([chosen[:SUBLANES], chosen[:SUBLANES]], axis=0)
        out = out + matmul_tn(both, mask)
        for c in range(2):
            for k in range(per):
                value = out[c * length : (c + 1) * length, k * length : (k + 1) * length]
                send[:, k, c, node] = value.reshape(grid_size, grid_part, length)
        return carry

    def copy_of(at, j):
        nodes = pl.ds(at * group, group)
        return pltpu.make_async_remote_copy(
            src_ref=send.at[order[j], :, :, nodes],
            dst_ref=out_ref.at[me, :, :, nodes],
            send_sem=sems.at[0, at, j],
            recv_sem=sems.at[1, at, j],
            device_id={"grid": order[j]},
            device_id_type=MESH,
        )

    groups = count // group
    for at in range(groups):
        lax.fori_loop(at * group, (at + 1) * group, to_slabs, 0)
        for j in range(grid_size - 1):
            copy_of(at, j).start()
    own = pltpu.make_async_copy(send.at[me], out_ref.at[me], sems.at[0, groups, 0])
    own.start()
    own.wait()
    for at in range(groups):
        for j in range(grid_size - 1):
            copy_of(at, j).wait()


def right_triple(ti_ref):
    wide = ti_ref.shape[1] // 3
    high, low = ti_ref[:, 0:wide], ti_ref[:, wide : 2 * wide]
    return jnp.concatenate([high, high, low], axis=1)


def middle(waves, shell, frac, pair_shell, pair_frac, kernel_table, tables, planes, grid_size):
    count = kernel_table.shape[0]
    length = waves.shape[-1]
    per = planes // grid_size
    padded = -(-count // SUBLANES) * SUBLANES
    depth = -(-(kernel_table.shape[2]) // LANES) * LANES
    table = jnp.pad(kernel_table, ((0, 0), (0, padded - count), (0, depth - kernel_table.shape[2])))
    table = table.reshape(count * padded, depth)
    rounded = lax.reduce_precision(table, exponent_bits=8, mantissa_bits=7)
    high, low = rounded.astype(jnp.bfloat16), (table - rounded).astype(jnp.bfloat16)
    table = jnp.concatenate([high, low, high], axis=1)
    group = count // 4 if count % 4 == 0 else count
    sizes = (count, padded, grid_size, planes, length, group)
    grid_part = length // grid_size
    wide = per * length
    shape = (grid_size, per, 2, count, grid_part, length)
    return pl.pallas_call(
        lambda *refs: middle_kernel(sizes, *refs),
        in_specs=[pl.BlockSpec(memory_space=VMEM)] * 8,
        out_specs=pl.BlockSpec(memory_space=VMEM),
        out_shape=jax.ShapeDtypeStruct(shape, jnp.float32),
        scratch_shapes=[
            VMEM((count, 2 * length, wide), jnp.float32),
            VMEM((per, 2 * length * padded, length), jnp.float32),
            VMEM((count * padded, wide), jnp.float32),
            VMEM((2, padded * SUBLANES, length), jnp.float32),
            VMEM(shape, jnp.float32),
            pltpu.SemaphoreType.DMA((2, count // group + 1, grid_size - 1)),
        ],
        compiler_params=pltpu.CompilerParams(
            collective_id=2, has_side_effects=True, vmem_limit_bytes=60 * 2**20
        ),
    )(waves, shell, frac, pair_shell, pair_frac, table, tables["x_forward"], tables["x_backward"])


def last_kernel(sizes, back_ref, index_ref, slope_ref, tz_ref, ty_ref, out_ref, slab, turned, ids):
    count, planes, grid_part, length = sizes
    band_at = lax.axis_index("band")
    rows = count * grid_part

    def to_rows(plane, carry):
        kind = jnp.minimum(plane + band_at * planes, 1)
        parts = 4
        size = rows // parts
        for at in range(parts):
            left = jnp.concatenate(
                [back_ref[plane, c, at * size : (at + 1) * size, :] for c in range(2)], axis=1
            )
            out = matmul(triple_left(left), ty_ref[kind])
            for c in range(2):
                start = pl.multiple_of((c * planes + plane) * rows + at * size, SUBLANES)
                slab[pl.ds(start, size), :] = out[:, c * length : (c + 1) * length]
        return carry

    lax.fori_loop(0, planes, to_rows, 0)
    table = tz_ref[band_at]

    def pair_of(pair, carry):
        for side in range(2):
            x_at = pair * 2 + side
            lanes = slice(side * length, (side + 1) * length)
            ids[:, lanes] = index_ref[x_at].T - 1
            for j in range(4):
                turned[j, :, lanes] = slope_ref[j, x_at].T

        def add_node(node, total):
            start = node * grid_part + pair * 2
            sides = []
            for side in range(2):
                parts = [
                    slab[pl.ds(c * planes * rows + start + side, planes, stride=rows), :]
                    for c in range(2)
                ]
                sides.append(jnp.concatenate(parts, axis=0))
            field = matmul(table, triple_right(jnp.concatenate(sides, axis=1)))
            index = ids[...]
            slope = jnp.where(index == node, turned[0], 0.0)
            for j in range(1, 4):
                slope = jnp.where(index == node - j, turned[j], slope)
            return total + field * slope

        total = lax.fori_loop(0, count, add_node, jnp.zeros((length, 2 * length), jnp.float32))
        for side in range(2):
            out_ref[pair * 2 + side] = total[:, side * length : (side + 1) * length].T
        return carry

    lax.fori_loop(0, grid_part // 2, pair_of, 0)


def last(returned, node_index, node_slope, tables, count, planes):
    grid_part, length = node_index.shape[:2]
    sizes = (count, planes, grid_part, length)
    rows = count * grid_part
    returned = returned.reshape(planes, 2, rows, length)
    return pl.pallas_call(
        lambda *refs: last_kernel(sizes, *refs),
        in_specs=[pl.BlockSpec(memory_space=VMEM)] * 5,
        out_specs=pl.BlockSpec(memory_space=VMEM),
        out_shape=jax.ShapeDtypeStruct(node_index.shape, jnp.float32),
        scratch_shapes=[
            VMEM((2 * planes * rows, length), jnp.float32),
            VMEM((4, length, 2 * length), jnp.float32),
            VMEM((length, 2 * length), jnp.int32),
        ],
        compiler_params=pltpu.CompilerParams(vmem_limit_bytes=60 * 2**20),
    )(returned, node_index, node_slope, tables["z_backward"], tables["y_backward"])


def fused_per_device(tables, partial_density, node_index, node_weight, node_slope, kernel_table):
    length = node_index.shape[1]
    half = length // 2
    count = kernel_table.shape[0]
    planes = half // lax.axis_size("band")
    grid_size = lax.axis_size("grid")
    per = planes // grid_size
    band_at, grid_at = lax.axis_index("band"), lax.axis_index("grid")
    density = band_sum(partial_density[0], 0)
    waves = forward(density, node_index, node_weight, tables, count, planes, grid_size)

    full_range = jnp.arange(length, dtype=jnp.int32)
    own_planes = band_at * planes + grid_at * per + jnp.arange(per, dtype=jnp.int32)
    freq = frequency_of(full_range, length)
    third = jnp.where(
        (own_planes[:, None] == 0) & (full_range[None] > half),
        half * half,
        (own_planes * own_planes)[:, None],
    )
    base = (third + (freq * freq)[None]).reshape(per * length)
    steps = jnp.arange(half + 1, dtype=jnp.int32)
    shell, frac = shell_split(base[None] + (steps * steps)[:, None])
    pair = jnp.concatenate([freq * freq, freq * freq + half * half])
    pair = jnp.pad(pair, (0, per * length - 2 * length))
    pair_shell, pair_frac = shell_split(jnp.stack([pair, pair + half * half]))
    returned = middle(
        waves, shell, frac, pair_shell, pair_frac, kernel_table, tables, planes, grid_size
    )
    potential = last(returned, node_index, node_slope, tables, count, planes)
    return band_sum(potential, 3)


def fits(mesh, length, groups):
    bands, grids = mesh.shape["band"], mesh.shape["grid"]
    planes = length // 2 // bands
    return (
        length == LANES
        and planes == SUBLANES
        and planes % grids == 0
        and planes // grids >= 2
        and bands % 2 == 0
        and (length // grids) % max(SUBLANES, bands) == 0
    )


def solution(mesh):
    placed = (
        P("band", "grid", None, None),
        P("grid", None, None),
        P(None, "grid", None, None),
        P(None, "grid", None, None),
        P(),
    )

    def program(*args):
        length = args[1].shape[0]
        body = per_device
        if fits(mesh, length, args[0].shape[0]):
            bands = mesh.shape["band"]
            tables = constant_tables(length, bands, length // 2 // bands)
            tables = {name: jnp.asarray(table) for name, table in tables.items()}
            body = lambda *blocks: fused_per_device(tables, *blocks)
        return jax.shard_map(
            body, mesh=mesh, in_specs=placed, out_specs=P("grid", None, None), check_vma=False
        )(*args)

    return program
```

```python
import math

import jax
import jax.numpy as jnp
import numpy as np
from jax import lax
from jax.experimental import pallas as pl
from jax.experimental.pallas import tpu as pltpu
from jax.sharding import PartitionSpec as P

def frequency_of(positions, length):
    return jnp.where(positions < length // 2, positions, positions - length)


def shell_split(square_norm):
    root_value = jnp.sqrt(square_norm.astype(jnp.float32))
    shell_idx = root_value.astype(jnp.int32)
    shell_idx = shell_idx - (shell_idx * shell_idx > square_norm).astype(jnp.int32)
    shell_idx = shell_idx + ((shell_idx + 1) * (shell_idx + 1) <= square_norm).astype(jnp.int32)
    fraction = root_value - shell_idx.astype(jnp.float32)
    return (shell_idx, fraction)


def node_fields(count_nodes, intervals, weights):
    node_ids = jnp.arange(count_nodes, dtype=jnp.int32)
    summed = jnp.zeros((count_nodes,) + intervals.shape, jnp.float32)
    for offset in range(4):
        matched = node_ids[:, None, None, None] == (intervals + (offset - 1))[None]
        summed = summed + jnp.where(matched, weights[offset][None], jnp.zeros((), jnp.float32))
    return summed


def phase_table(source_idx, target_idx, modulus):
    product_mod = source_idx[:, None] * target_idx[None, :] % modulus
    angles = product_mod.astype(jnp.float32) * (2.0 * math.pi / modulus)
    return (jnp.cos(angles), jnp.sin(angles))


def contract(pattern, operand, matrix):
    return jnp.einsum(pattern, operand, matrix, precision=lax.Precision.HIGHEST)


def mirrored(values, dim):
    return jnp.roll(jnp.flip(values, dim), 1, dim)


def forward_tables(positions, plane_ids, length):
    cosine, sine = phase_table(positions, plane_ids, length)
    alternating = jnp.where(positions % 2 == 0, 1.0, -1.0).astype(jnp.float32)
    sine = jnp.where(plane_ids[None, :] == 0, -alternating[:, None], sine)
    return (cosine, sine)


def shell_weights_of(square_norm, shell_count):
    shell_ids = jnp.arange(shell_count, dtype=jnp.int32)
    shell_idx, fraction = shell_split(square_norm)
    expand = (slice(None),) + (None,) * square_norm.ndim
    lower_hit = shell_ids[expand] == shell_idx[None]
    upper_hit = shell_ids[expand] == shell_idx[None] + 1
    return jnp.where(lower_hit, 1.0 - fraction[None], 0.0) + jnp.where(
        upper_hit, fraction[None], 0.0
    )


def short(pattern, left, right):
    return jnp.einsum(pattern, left, right, precision=lax.Precision.HIGH)


def halves(values):
    high = values.astype(jnp.bfloat16)
    low = (values - high.astype(jnp.float32)).astype(jnp.bfloat16)
    return high, low


def mix_kernel(count, padded, shell_ref, frac_ref, table_ref, spec_ref, out_ref):
    rows, lanes = shell_ref.shape[1:]
    ids = lax.broadcasted_iota(jnp.int32, (table_ref.shape[1] // 3, lanes), 0)

    def hats(row):
        shell = shell_ref[0, pl.ds(row, 1), :]
        frac = frac_ref[0, pl.ds(row, 1), :]
        return jnp.where(ids == shell, 1.0 - frac, jnp.where(ids == shell + 1, frac, 0.0))

    def step(pair, carry):
        both = jnp.concatenate([hats(2 * pair), hats(2 * pair + 1)], axis=1)
        high, low = halves(both)
        phi = jnp.dot(
            table_ref[...],
            jnp.concatenate([high, high, low], axis=0),
            preferred_element_type=jnp.float32,
        )
        for side in range(2):
            row = 2 * pair + side
            real = jnp.zeros((padded, lanes), jnp.float32)
            imag = jnp.zeros((padded, lanes), jnp.float32)
            for node in range(count):
                part = phi[node * padded : (node + 1) * padded, side * lanes : (side + 1) * lanes]
                real = real + part * spec_ref[0, node, 0, pl.ds(row, 1), :]
                imag = imag + part * spec_ref[1, node, 0, pl.ds(row, 1), :]
            out_ref[0, row, 0] = real[:count]
            out_ref[0, row, 1] = imag[:count]
        return carry

    lax.fori_loop(0, rows // 2, step, 0)


def mix(spectrum, shell, frac, kernel_table):
    _, count, planes, rows, lanes = spectrum.shape
    padded = -(-count // 8) * 8
    depth = -(-(kernel_table.shape[2]) // 128) * 128
    table = jnp.pad(kernel_table, ((0, 0), (0, padded - count), (0, depth - kernel_table.shape[2])))
    table = table.reshape(count * padded, depth)
    rounded = lax.reduce_precision(table, exponent_bits=8, mantissa_bits=7)
    high, low = rounded.astype(jnp.bfloat16), (table - rounded).astype(jnp.bfloat16)
    table = jnp.concatenate([high, low, high], axis=1)
    return pl.pallas_call(
        lambda *refs: mix_kernel(count, padded, *refs),
        grid=(planes,),
        in_specs=[
            pl.BlockSpec((1, rows, lanes), lambda p: (p, 0, 0)),
            pl.BlockSpec((1, rows, lanes), lambda p: (p, 0, 0)),
            pl.BlockSpec(table.shape, lambda p: (0, 0)),
            pl.BlockSpec((2, count, 1, rows, lanes), lambda p: (0, 0, p, 0, 0)),
        ],
        out_specs=pl.BlockSpec((1, rows, 2, count, lanes), lambda p: (p, 0, 0, 0, 0)),
        out_shape=jax.ShapeDtypeStruct((planes, rows, 2, count, lanes), jnp.float32),
    )(shell, frac, table, spectrum)


def per_device(partial_density, node_index, node_weight, node_slope, kernel_table):
    length = node_index.shape[1]
    half = length // 2
    count_nodes = kernel_table.shape[0]
    shell_count = kernel_table.shape[2]
    planes = half // lax.axis_size("band")
    grid_size = lax.axis_size("grid")
    grid_part = length // grid_size
    band_at = lax.axis_index("band")
    grid_at = lax.axis_index("grid")
    full_range = jnp.arange(length, dtype=jnp.int32)
    own_planes = band_at * planes + jnp.arange(planes, dtype=jnp.int32)
    own_rows = grid_at * grid_part + jnp.arange(grid_part, dtype=jnp.int32)
    lower = ((full_range >= 1) & (full_range < half)).astype(jnp.float32)
    upper = (full_range > half).astype(jnp.float32)
    single = 1.0 - lower - upper
    joint = (own_planes == 0)[:, None, None, None, None]
    cosine, sine = phase_table(full_range, full_range, length)
    forward = jnp.stack(
        [jnp.stack([cosine, -sine], 1), jnp.stack([sine, cosine], 1)]
    )
    low_only = lower + single
    packed = jnp.stack(
        [
            jnp.stack([cosine * low_only, -sine * lower], 1),
            jnp.stack([cosine * upper, -sine * upper + cosine * single], 1),
        ]
    )
    forward_y = jnp.where(joint, packed[None], forward[None])
    backward = jnp.stack(
        [jnp.stack([cosine, sine], 1), jnp.stack([-sine, cosine], 1)]
    )
    lower_col, upper_col, single_col = (v[:, None] for v in (lower, upper, single))
    opened = jnp.stack(
        [
            jnp.stack([cosine * (2.0 * lower_col + single_col), cosine * (2.0 * upper_col)], 1),
            jnp.stack(
                [sine * (-2.0 * lower_col), sine * (-2.0 * upper_col) + cosine * single_col], 1
            ),
        ]
    )
    backward_y = jnp.where(joint, opened[None], backward[None])

    density = lax.psum(partial_density[0], "band")
    theta_fields = density[None] * node_fields(count_nodes, node_index, node_weight)
    cosine_z, sine_z = forward_tables(full_range, own_planes, length)
    table_z = jnp.stack([cosine_z, -sine_z], 1)
    columns = short("zcp,axyz->cpaxy", table_z, theta_fields)
    waves = short("cpaxy,pcydw->wdapx", columns, forward_y)
    waves = waves.reshape((grid_size, grid_part) + waves.shape[1:])
    pencils = lax.all_to_all(waves, "grid", split_axis=0, concat_axis=0, tiled=True)
    forward_x = forward.reshape((2, grid_size, grid_part) + forward.shape[2:])
    spectrum = short("gwdapx,dgxev->eapwv", pencils, forward_x)

    freq_x = frequency_of(full_range, length)
    square_x = freq_x * freq_x
    freq_rows = frequency_of(own_rows, length)
    square_rows = freq_rows * freq_rows
    third_square = jnp.where(
        (own_planes[:, None] == 0) & (own_rows[None, :] > half),
        half * half,
        (own_planes * own_planes)[:, None],
    )
    square_norm = (third_square + square_rows[None, :])[:, :, None] + square_x
    shell, frac = shell_split(square_norm)
    mixed = mix(spectrum, shell, frac, kernel_table)

    flag = ((own_rows[0] == 0) | (own_rows[0] == half)) & (own_planes[0] == 0)
    first_norm = square_x + square_rows[0]
    pair_norm = jnp.stack([first_norm, first_norm + half * half])
    kernels = contract("abs,sqx->qabx", kernel_table, shell_weights_of(pair_norm, shell_count))
    spread = (0.5 * flag.astype(jnp.float32)) * (kernels[0] - kernels[1])
    base = spectrum[:, :, 0, 0, :]
    turned = mirrored(base, 2)
    delta = jnp.stack([turned[0] - base[0], -turned[1] - base[1]])
    extra = jnp.sum(spread[None] * delta[:, :, None, :], axis=1)
    mixed = mixed.at[0, 0].add(extra)

    backward_x = backward.reshape(2, length, 2, grid_size, grid_part)
    inverse = short("pwdbv,dvegx->gwebpx", mixed, backward_x)
    returned = lax.all_to_all(inverse, "grid", split_axis=0, concat_axis=0, tiled=True)
    backward_y = backward_y.reshape((planes, 2, grid_size, grid_part, 2, length))
    slab = short("gwdbpx,pdgwcy->cpbxy", returned, backward_y)
    cosine_own, sine_own = phase_table(own_planes, full_range, length)
    alternating = jnp.where(full_range % 2 == 0, 1.0, -1.0).astype(jnp.float32)
    cosine_back = jnp.where(own_planes[:, None] == 0, 1.0, 2.0 * cosine_own)
    sine_back = jnp.where(own_planes[:, None] == 0, -alternating[None, :], 2.0 * sine_own)
    table_back = jnp.stack([cosine_back, -sine_back]) * (1.0 / float(length) ** 3)
    field_parts = short("cpbxy,cpz->bxyz", slab, table_back)
    slopes = node_fields(count_nodes, node_index, node_slope)
    partial_potential = jnp.sum(field_parts * slopes, axis=0)
    return lax.psum(partial_potential, "band")


LANES = 128
SUBLANES = 8
MESH = pl.DeviceIdType.MESH
VMEM = pltpu.VMEM


def split_table(table):
    high = np.asarray(table).astype(jnp.bfloat16)
    low = (np.asarray(table) - high.astype(np.float64)).astype(jnp.bfloat16)
    return high, low


def angles_of(sources, targets, length):
    phase = (np.outer(sources, targets) % length) * (2.0 * np.pi / length)
    return np.cos(phase), np.sin(phase)


def complex_table(cosine, sine):
    return np.stack([np.stack([cosine, -sine], 1), np.stack([sine, cosine], 1)])


def constant_tables(length, bands, planes):
    points = np.arange(length)
    half = length // 2
    cosine, sine = angles_of(points, points, length)
    lower = ((points >= 1) & (points < half)).astype(np.float64)
    upper = (points > half).astype(np.float64)
    single = 1.0 - lower - upper
    forward = complex_table(cosine, sine)
    backward = complex_table(cosine, -sine)
    packed = np.stack(
        [
            np.stack([cosine * (lower + single), -sine * lower], 1),
            np.stack([cosine * upper, -sine * upper + cosine * single], 1),
        ]
    )
    lo, up, one = (v[:, None] for v in (lower, upper, single))
    opened = np.stack(
        [
            np.stack([cosine * (2 * lo + one), cosine * (2 * up)], 1),
            np.stack([sine * (-2 * lo), sine * (-2 * up) + cosine * one], 1),
        ]
    )
    square = (2 * length, 2 * length)

    def right(table):
        high, low = split_table(table.reshape(square))
        return np.concatenate([high, high, low], 0)

    def left(table):
        high, low = split_table(table.reshape(square).T)
        return np.concatenate([high, low, high], 1)

    alternating = np.where(points % 2 == 0, 1.0, -1.0)
    z_forward, z_backward = [], []
    for band in range(bands):
        ids = band * planes + np.arange(planes)
        cos_z, sin_z = angles_of(ids, points, length)
        minus = np.where(ids[:, None] == 0, alternating[None], -sin_z)
        rows = np.concatenate([cos_z, minus], 0)
        high, low = split_table(rows)
        top = np.concatenate([high, high], 1)
        bottom = np.concatenate([low, np.zeros_like(low)], 1)
        z_forward.append(np.concatenate([top, bottom], 0))
        first = ids[:, None] == 0
        rows = np.concatenate(
            [np.where(first, 1.0, 2.0 * cos_z), np.where(first, alternating[None], -2.0 * sin_z)]
        ) / float(length) ** 3
        high, low = split_table(rows.T)
        z_backward.append(np.concatenate([high, low, high], 1))
    return {
        "y_forward": np.stack([right(packed), right(forward)]),
        "y_backward": np.stack([right(opened), right(backward)]),
        "x_forward": left(forward),
        "x_backward": left(backward),
        "z_forward": np.stack(z_forward),
        "z_backward": np.stack(z_backward),
    }


def triple_left(values):
    high, low = halves(values)
    return jnp.concatenate([high, low, high], axis=1)


def triple_right(values):
    high, low = halves(values)
    return jnp.concatenate([high, high, low], axis=0)


def matmul(left, right):
    return jnp.dot(left, right, preferred_element_type=jnp.float32)


def matmul_nt(left, right):
    return lax.dot_general(
        left, right, (((1,), (1,)), ((), ())), preferred_element_type=jnp.float32
    )


def matmul_tn(left, right):
    return lax.dot_general(
        left, right, (((0,), (0,)), ((), ())), preferred_element_type=jnp.float32
    )


def greet(targets):
    barrier = pltpu.get_barrier_semaphore()
    for axis, target in targets:
        pl.semaphore_signal(barrier, inc=1, device_id={axis: target}, device_id_type=MESH)
    pl.semaphore_wait(barrier, len(targets))


class BandSum:
    def __init__(self, outer, chunk_rows, src, dst, near_buf, stage, far_buf, sems):
        me = lax.axis_index("band")
        self.outer, self.src, self.dst = outer, src, dst
        self.near_buf, self.stage, self.far_buf, self.sems = near_buf, stage, far_buf, sems
        self.far, self.near = me // 2, lax.rem(me, 2)
        self.partner = self.far * 2 + (1 - self.near)
        self.others = [lax.rem(self.far + 1 + j, outer) for j in range(outer)]
        self.back = [lax.rem(self.far + outer - 1 - j, outer) for j in range(outer)]
        self.chunk_rows = chunk_rows
        self.side_rows = chunk_rows // 2
        self.part = self.side_rows // outer
        self.peers = [("band", self.partner)] + [
            ("band", o * 2 + self.near) for o in self.others[:-1]
        ]

    def piece(self, chunk, side, quarter):
        start = chunk * self.chunk_rows + side * self.side_rows + quarter * self.part
        return pl.ds(start, self.part)

    def copy(self, src, dst, chunk, kind, j, target):
        return pltpu.make_async_remote_copy(
            src_ref=src,
            dst_ref=dst,
            send_sem=self.sems.at[chunk, kind, 0, j],
            recv_sem=self.sems.at[chunk, kind, 1, j],
            device_id={"band": target},
            device_id_type=MESH,
        )

    def near_copy(self, c, j):
        src = self.src.at[self.piece(c, 1 - self.near, self.others[j])]
        return self.copy(src, self.near_buf.at[c, j], c, 0, j, self.partner)

    def far_copy(self, c, j):
        target = self.others[j] * 2 + self.near
        return self.copy(self.stage.at[c, j], self.far_buf.at[c, j], c, 1, j, target)

    def gather_copy(self, c, j):
        own = self.dst.at[self.piece(c, self.near, self.far)]
        return self.copy(own, own, c, 2, j, self.others[j] * 2 + self.near)

    def pass_copy(self, c, j):
        block = self.dst.at[self.piece(c, self.near, self.back[j])]
        return self.copy(block, block, c, 3, j, self.partner)

    def start(self, c):
        for j in range(self.outer):
            self.near_copy(c, j).start()

    def reduce(self, c):
        for j in range(self.outer - 1):
            self.near_copy(c, j).wait_recv()
            mine = self.src[self.piece(c, self.near, self.others[j])]
            self.stage[c, j] = mine + self.near_buf[c, j]
            self.far_copy(c, j).start()

    def finish(self, c):
        last = self.outer - 1
        self.near_copy(c, last).wait_recv()
        own = self.piece(c, self.near, self.far)
        total = self.src[own] + self.near_buf[c, last]
        for j in range(last):
            self.far_copy(c, j).wait_recv()
            total = total + self.far_buf[c, j]
        self.dst[own] = total
        for j in range(last):
            self.gather_copy(c, j).start()
        self.pass_copy(c, last).start()

    def forward(self, c):
        for j in range(self.outer - 1):
            self.gather_copy(c, j).wait_recv()
            self.pass_copy(c, j).start()

    def arrive(self, c):
        for j in range(self.outer):
            self.pass_copy(c, j).wait_recv()

    def drain(self, c):
        for j in range(self.outer):
            self.near_copy(c, j).wait_send()
            self.pass_copy(c, j).wait_send()
        for j in range(self.outer - 1):
            self.far_copy(c, j).wait_send()
            self.gather_copy(c, j).wait_send()


def band_scratch(outer, chunks, shape):
    part = (shape[0] // chunks // (2 * outer),) + shape[1:]
    return [
        VMEM((chunks, outer) + part, jnp.float32),
        VMEM((chunks, outer - 1) + part, jnp.float32),
        VMEM((chunks, outer - 1) + part, jnp.float32),
        pltpu.SemaphoreType.DMA((chunks, 4, 2, outer)),
    ]


def forward_kernel(
    sizes,
    partial_ref,
    index_hbm,
    weight_hbm,
    tz_ref,
    ty_ref,
    out_ref,
    density_ref,
    index_ref,
    weight_ref,
    theta,
    columns,
    send,
    sems,
    load_sems,
    *band_refs,
):
    count, grid_size, steps, planes, length, outer = sizes
    index_load = pltpu.make_async_copy(index_hbm, index_ref, load_sems.at[0])
    weight_load = pltpu.make_async_copy(weight_hbm, weight_ref, load_sems.at[1])
    band = BandSum(outer, SUBLANES, partial_ref, density_ref, *band_refs)
    step_rows = SUBLANES * length
    band_at, me = lax.axis_index("band"), lax.axis_index("grid")
    order = [lax.rem(me + 1 + j, grid_size) for j in range(grid_size)]
    per = planes // grid_size
    rows = count * SUBLANES
    greet(band.peers + [("grid", target) for target in order[:-1]])
    for step in range(steps):
        band.start(step)
    index_load.start()
    weight_load.start()

    def copy_of(step, slot, j):
        return pltpu.make_async_remote_copy(
            src_ref=send.at[slot, j],
            dst_ref=out_ref.at[:, :, me * steps + step],
            send_sem=sems.at[0, step, j],
            recv_sem=sems.at[1, step, j],
            device_id={"grid": order[j]},
            device_id_type=MESH,
        )

    def fill(step):
        block = 32

        def body(at, carry):
            x_at = step * SUBLANES + at // (length // block)
            start = pl.multiple_of(lax.rem(at, length // block) * block, block)
            place = pl.ds(pl.multiple_of(at * block, block), block)
            index = index_ref[x_at, pl.ds(start, block), :] - 1
            amount = density_ref[x_at, pl.ds(start, block), :]
            parts = [amount * weight_ref[j, x_at, pl.ds(start, block), :] for j in range(4)]
            for node in range(count):
                value = jnp.where(index == node, parts[0], 0.0)
                for j in range(1, 4):
                    value = jnp.where(index == node - j, parts[j], value)
                high, low = halves(value)
                theta[node, place, 0:length] = high
                theta[node, place, length : 2 * length] = low
            return carry

        lax.fori_loop(0, step_rows // block, body, 0)

    def columns_of(step):
        table = tz_ref[band_at]

        def body(node, carry):
            for pair in range(SUBLANES // 2):
                block = theta[node, pair * 2 * length : (pair + 1) * 2 * length, :]
                out = matmul_nt(table, block)
                out = out[: 2 * planes] + out[2 * planes :]
                for side in range(2):
                    for c in range(2):
                        row = c * planes * rows + node * SUBLANES + pair * 2 + side
                        columns[pl.ds(row, planes, stride=rows), :] = out[
                            c * planes : (c + 1) * planes, side * length : (side + 1) * length
                        ]
            return carry

        lax.fori_loop(0, count, body, 0)

    def waves_of(step, slot, j):
        for k in range(per):
            plane = order[j] * per + k
            start = pl.multiple_of(plane * rows, rows)
            left = jnp.concatenate(
                [columns[pl.ds(c * planes * rows + start, rows), :] for c in range(2)], axis=1
            )
            kind = jnp.minimum(plane + band_at * planes, 1)
            out = matmul(triple_left(left), ty_ref[kind])
            for d in range(2):
                value = out[:, d * length : (d + 1) * length]
                if j < grid_size - 1:
                    send[slot, j, k, d] = value
                else:
                    out_ref[k, d, me * steps + step] = value

    todo = []
    for at in range(steps + 3):
        for call, lag in ((band.reduce, 0), (band.finish, 1), (band.forward, 2)):
            if 0 <= at - lag < steps:
                todo.append((call, at - lag))
    ahead = todo.index((band.forward, 0)) + 1

    def advance(number):
        for call, chunk in todo[:number]:
            call(chunk)
        del todo[:number]

    advance(ahead)
    index_load.wait()
    weight_load.wait()
    for step in range(steps):
        slot = step % 2
        band.arrive(step)
        fill(step)
        advance(1)
        columns_of(step)
        for j in range(grid_size):
            advance(1 if step == 0 else len(todo))
            if step >= 2 and j < grid_size - 1:
                copy_of(step - 2, slot, j).wait_send()
            waves_of(step, slot, j)
            if j < grid_size - 1:
                copy_of(step, slot, j).start()
    for step in range(steps):
        band.drain(step)
        for j in range(grid_size - 1):
            if step >= steps - 2:
                copy_of(step, step % 2, j).wait_send()
            copy_of(step, step % 2, j).wait_recv()


def forward(partial, node_index, node_weight, tables, count, planes, grid_size):
    grid_part, length = partial.shape[:2]
    outer = lax.axis_size("band") // 2
    steps = grid_part // SUBLANES
    per = planes // grid_size
    sizes = (count, grid_size, steps, planes, length, outer)
    rows = count * SUBLANES
    whole = pl.BlockSpec(memory_space=VMEM)
    anywhere = pl.BlockSpec(memory_space=pl.ANY)
    return pl.pallas_call(
        lambda *refs: forward_kernel(sizes, *refs),
        in_specs=[whole, anywhere, anywhere, whole, whole],
        out_specs=whole,
        out_shape=jax.ShapeDtypeStruct(
            (per, 2, grid_size * steps, rows, length), jnp.float32
        ),
        scratch_shapes=[
            VMEM(partial.shape, jnp.float32),
            VMEM(node_index.shape, jnp.int32),
            VMEM(node_weight.shape, jnp.float32),
            VMEM((count, SUBLANES * length, 2 * length), jnp.bfloat16),
            VMEM((2 * planes * rows, length), jnp.float32),
            VMEM((2, grid_size - 1, per, 2, rows, length), jnp.float32),
            pltpu.SemaphoreType.DMA((2, steps, grid_size - 1)),
            pltpu.SemaphoreType.DMA((2,)),
        ]
        + band_scratch(outer, steps, partial.shape),
        compiler_params=pltpu.CompilerParams(
            collective_id=1, has_side_effects=True, vmem_limit_bytes=60 * 2**20
        ),
    )(partial, node_index, node_weight, tables["z_forward"], tables["y_forward"])


def middle_kernel(
    sizes,
    waves_ref,
    shell_ref,
    frac_ref,
    pair_shell_ref,
    pair_frac_ref,
    table_ref,
    tx_ref,
    ti_ref,
    index_hbm,
    slope_hbm,
    tz_ref,
    ty_ref,
    out_ref,
    spec,
    mixed,
    phi,
    extra,
    send,
    back,
    index_ref,
    slope_ref,
    slab,
    turned,
    ids_ref,
    fields,
    total_ref,
    potential,
    sems,
    load_sems,
    *band_refs,
):
    count, padded, grid_size, planes, length, outer = sizes
    index_load = pltpu.make_async_copy(index_hbm, index_ref, load_sems.at[0])
    slope_load = pltpu.make_async_copy(slope_hbm, slope_ref, load_sems.at[1])
    index_load.start()
    slope_load.start()
    band = BandSum(outer, SUBLANES, potential, out_ref, *band_refs)
    per = planes // grid_size
    grid_part = length // grid_size
    wide = per * length
    half = length // 2
    band_at, me = lax.axis_index("band"), lax.axis_index("grid")
    order = [lax.rem(me + 1 + j, grid_size) for j in range(grid_size)]
    steps = grid_part // SUBLANES
    rows = count * SUBLANES
    joint = (band_at == 0) & (me == 0)
    greet(band.peers + [("grid", target) for target in order[:-1]])

    lane = lax.broadcasted_iota(jnp.int32, (16, wide), 1)
    slot = lax.broadcasted_iota(jnp.int32, (16, wide), 0)
    chosen = jnp.where(lane == slot * half, 1.0, 0.0)
    chosen = jnp.where(slot < 2, chosen, 0.0).astype(jnp.bfloat16)

    def block_of(node, d):
        parts = [
            waves_ref[k, d, :, pl.ds(pl.multiple_of(node * SUBLANES, SUBLANES), SUBLANES), :]
            for k in range(per)
        ]
        return jnp.concatenate([p.reshape(length, length) for p in parts], axis=1)

    def to_spectrum(node, carry):
        values = jnp.concatenate([block_of(node, 0), block_of(node, 1)], axis=0)
        spec[node] = matmul(tx_ref[...], triple_right(values))
        return carry

    lax.fori_loop(0, count, to_spectrum, 0)

    ids = lax.broadcasted_iota(jnp.int32, (table_ref.shape[1] // 3, wide), 0)

    def hats(shell, frac):
        return jnp.where(ids == shell, 1.0 - frac, jnp.where(ids == shell + 1, frac, 0.0))

    def mix_rows(row_sets, load):
        sums = [jnp.zeros((padded, wide), jnp.float32) for _ in range(2 * len(row_sets))]
        for node in range(count):
            part = phi[node * padded : (node + 1) * padded, :]
            for at, row in enumerate(row_sets):
                for e in range(2):
                    sums[2 * at + e] = sums[2 * at + e] + part * load(node, e, row)
        return sums

    def step(i, carry):
        weights = hats(shell_ref[pl.ds(i, 1), :], frac_ref[pl.ds(i, 1), :])
        phi[...] = matmul(table_ref[...], triple_right(weights))
        rows = [i, lax.rem(length - i, length)]
        sums = mix_rows(rows, lambda node, e, row: spec[node, pl.ds(e * length + row, 1), :])
        for at, row in enumerate(rows):
            for e in range(2):
                start = pl.multiple_of((e * length + row) * padded, SUBLANES)
                for k in range(per):
                    value = sums[2 * at + e][:, k * length : (k + 1) * length]
                    mixed[k, pl.ds(start, padded), :] = value
        return carry

    lax.fori_loop(0, half + 1, step, 0)

    extra[...] = jnp.zeros_like(extra)

    @pl.when(joint)
    def _():
        right = jnp.concatenate(
            [tx_ref[:, length : 2 * length], tx_ref[:, 3 * length : 4 * length]], axis=1
        )

        def gather(node, carry):
            high, low = halves(block_of(node, 1))
            imag = (matmul_nt(chosen, high) + matmul_nt(chosen, low))[:SUBLANES]
            high, low = halves(-2.0 * imag)
            zero = jnp.zeros_like(low)
            left = jnp.concatenate(
                [jnp.concatenate([high, high], 1), jnp.concatenate([low, zero], 1)], axis=0
            )
            delta = matmul_nt(left, right)
            delta = delta[:SUBLANES] + delta[SUBLANES:]
            spec[node, 0:SUBLANES, :] = delta
            return carry

        lax.fori_loop(0, count, gather, 0)
        weights = 0.5 * (
            hats(pair_shell_ref[0:1, :], pair_frac_ref[0:1, :])
            - hats(pair_shell_ref[1:2, :], pair_frac_ref[1:2, :])
        )
        phi[...] = matmul(table_ref[...], triple_right(weights))

        def load(node, e, row):
            return jnp.concatenate(
                [spec[node, r : r + 1, e * length : (e + 1) * length] for r in range(2)], axis=1
            )

        real, imag = mix_rows([0], load)
        for r in range(2):
            left = jnp.concatenate(
                [real[:, r * length : (r + 1) * length], imag[:, r * length : (r + 1) * length]],
                axis=1,
            )
            added = matmul_nt(triple_left(left), right_triple(ti_ref))
            for c in range(2):
                value = added[:, c * length : (c + 1) * length]
                extra[c, pl.ds(r, padded, stride=SUBLANES), :] = value

    def to_slabs(node, carry):
        rows = [mixed[k, pl.ds(node, 2 * length, stride=padded), :] for k in range(per)]
        out = matmul(ti_ref[...], triple_right(jnp.concatenate(rows, axis=1)))
        place = pl.ds(pl.multiple_of(node * SUBLANES, SUBLANES), SUBLANES)
        high, low = halves(jnp.concatenate([extra[c, place, :] for c in range(2)], axis=1))
        both = jnp.concatenate([high, low], axis=0)
        mask = jnp.concatenate([chosen[:SUBLANES], chosen[:SUBLANES]], axis=0)
        out = out + matmul_tn(both, mask)
        for c in range(2):
            for k in range(per):
                value = out[c * length : (c + 1) * length, k * length : (k + 1) * length]
                value = value.reshape(grid_size, steps, SUBLANES, length)
                place = pl.ds(pl.multiple_of(node * SUBLANES, SUBLANES), SUBLANES)
                send[:, :, k, c, place, :] = value
        return carry

    def copy_of(step, j):
        return pltpu.make_async_remote_copy(
            src_ref=send.at[order[j], step],
            dst_ref=back.at[step, me],
            send_sem=sems.at[0, step, j],
            recv_sem=sems.at[1, step, j],
            device_id={"grid": order[j]},
            device_id_type=MESH,
        )

    def own_copy(step):
        return pltpu.make_async_copy(
            send.at[me, step], back.at[step, me], sems.at[0, step, grid_size - 1]
        )

    lax.fori_loop(0, count, to_slabs, 0)
    for step in range(steps):
        for j in range(grid_size - 1):
            copy_of(step, j).start()
        own_copy(step).start()
    index_load.wait()
    slope_load.wait()
    table = tz_ref[band_at]

    def y_rows(step):
        def body(plane, carry):
            kind = jnp.minimum(plane + band_at * planes, 1)
            left = jnp.concatenate(
                [back[step, plane // per, lax.rem(plane, per), c] for c in range(2)], axis=1
            )
            out = matmul(triple_left(left), ty_ref[kind])
            for c in range(2):
                start = pl.multiple_of((c * planes + plane) * rows, SUBLANES)
                slab[pl.ds(start, rows), :] = out[:, c * length : (c + 1) * length]
            return carry

        lax.fori_loop(0, planes, body, 0)

    def z_rows(step):
        def pair_of(pair, carry):
            first = step * SUBLANES + pair * 2
            for side in range(2):
                lanes = slice(side * length, (side + 1) * length)
                ids_ref[:, lanes] = index_ref[first + side].T - 1
                for j in range(4):
                    turned[j, :, lanes] = slope_ref[j, first + side].T
            for node in range(count):
                sides = []
                for side in range(2):
                    start = node * SUBLANES + pair * 2 + side
                    parts = [
                        slab[pl.ds(c * planes * rows + start, planes, stride=rows), :]
                        for c in range(2)
                    ]
                    sides.append(jnp.concatenate(parts, axis=0))
                fields[node] = matmul(table, triple_right(jnp.concatenate(sides, axis=1)))

            def pick(block, carry):
                place = pl.ds(pl.multiple_of(block * SUBLANES, SUBLANES), SUBLANES)
                index = ids_ref[place, :]
                picked = [jnp.zeros((SUBLANES, 2 * length), jnp.float32) for _ in range(4)]
                for node in range(count):
                    field = fields[node, place, :]
                    for j in range(4):
                        picked[j] = jnp.where(index == node - j, field, picked[j])
                summed = picked[0] * turned[0, place, :]
                for j in range(1, 4):
                    summed = summed + picked[j] * turned[j, place, :]
                total_ref[place, :] = summed
                return carry

            lax.fori_loop(0, length // SUBLANES, pick, 0)
            for side in range(2):
                lanes = slice(side * length, (side + 1) * length)
                potential[first + side] = total_ref[:, lanes].T
            return carry

        lax.fori_loop(0, SUBLANES // 2, pair_of, 0)

    calls = ((band.forward, 3), (band.finish, 2), (band.reduce, 1))
    for at in range(steps + 3):
        if at < steps:
            own_copy(at).wait()
            for j in range(grid_size - 1):
                copy_of(at, j).wait_recv()
            y_rows(at)
        for call, lag in calls:
            if 0 <= at - lag < steps:
                call(at - lag)
        if at < steps:
            z_rows(at)
            band.start(at)
    for step in range(steps):
        band.arrive(step)
        band.drain(step)
        for j in range(grid_size - 1):
            copy_of(step, j).wait_send()


def right_triple(ti_ref):
    wide = ti_ref.shape[1] // 3
    high, low = ti_ref[:, 0:wide], ti_ref[:, wide : 2 * wide]
    return jnp.concatenate([high, high, low], axis=1)


def backward(
    waves, shells, node_index, node_slope, kernel_table, tables, planes, grid_size
):
    count = kernel_table.shape[0]
    length = waves.shape[-1]
    outer = lax.axis_size("band") // 2
    per = planes // grid_size
    padded = -(-count // SUBLANES) * SUBLANES
    depth = -(-(kernel_table.shape[2]) // LANES) * LANES
    table = jnp.pad(kernel_table, ((0, 0), (0, padded - count), (0, depth - kernel_table.shape[2])))
    table = table.reshape(count * padded, depth)
    rounded = lax.reduce_precision(table, exponent_bits=8, mantissa_bits=7)
    high, low = rounded.astype(jnp.bfloat16), (table - rounded).astype(jnp.bfloat16)
    table = jnp.concatenate([high, low, high], axis=1)
    sizes = (count, padded, grid_size, planes, length, outer)
    grid_part = length // grid_size
    steps = grid_part // SUBLANES
    wide = per * length
    rows = count * SUBLANES
    whole = pl.BlockSpec(memory_space=VMEM)
    anywhere = pl.BlockSpec(memory_space=pl.ANY)
    return pl.pallas_call(
        lambda *refs: middle_kernel(sizes, *refs),
        in_specs=[whole] * 8 + [anywhere] * 2 + [whole] * 2,
        out_specs=whole,
        out_shape=jax.ShapeDtypeStruct(node_index.shape, jnp.float32),
        scratch_shapes=[
            VMEM((count, 2 * length, wide), jnp.float32),
            VMEM((per, 2 * length * padded, length), jnp.float32),
            VMEM((count * padded, wide), jnp.float32),
            VMEM((2, padded * SUBLANES, length), jnp.float32),
            VMEM((grid_size, steps, per, 2, rows, length), jnp.float32),
            VMEM((steps, grid_size, per, 2, rows, length), jnp.float32),
            VMEM(node_index.shape, jnp.int32),
            VMEM(node_slope.shape, jnp.float32),
            VMEM((2 * planes * rows, length), jnp.float32),
            VMEM((4, length, 2 * length), jnp.float32),
            VMEM((length, 2 * length), jnp.int32),
            VMEM((count, length, 2 * length), jnp.float32),
            VMEM((length, 2 * length), jnp.float32),
            VMEM(node_index.shape, jnp.float32),
            pltpu.SemaphoreType.DMA((2, steps, grid_size)),
            pltpu.SemaphoreType.DMA((2,)),
        ]
        + band_scratch(outer, steps, node_index.shape),
        compiler_params=pltpu.CompilerParams(
            collective_id=2, has_side_effects=True, vmem_limit_bytes=62 * 2**20
        ),
    )(
        waves,
        *shells,
        table,
        tables["x_forward"],
        tables["x_backward"],
        node_index,
        node_slope,
        tables["z_backward"],
        tables["y_backward"],
    )


def fused_per_device(tables, partial_density, node_index, node_weight, node_slope, kernel_table):
    length = node_index.shape[1]
    half = length // 2
    count = kernel_table.shape[0]
    planes = half // lax.axis_size("band")
    grid_size = lax.axis_size("grid")
    per = planes // grid_size
    band_at, grid_at = lax.axis_index("band"), lax.axis_index("grid")
    waves = forward(partial_density[0], node_index, node_weight, tables, count, planes, grid_size)

    full_range = jnp.arange(length, dtype=jnp.int32)
    own_planes = band_at * planes + grid_at * per + jnp.arange(per, dtype=jnp.int32)
    freq = frequency_of(full_range, length)
    third = jnp.where(
        (own_planes[:, None] == 0) & (full_range[None] > half),
        half * half,
        (own_planes * own_planes)[:, None],
    )
    base = (third + (freq * freq)[None]).reshape(per * length)
    steps = jnp.arange(half + 1, dtype=jnp.int32)
    shell, frac = shell_split(base[None] + (steps * steps)[:, None])
    pair = jnp.concatenate([freq * freq, freq * freq + half * half])
    pair = jnp.pad(pair, (0, per * length - 2 * length))
    pair_shell, pair_frac = shell_split(jnp.stack([pair, pair + half * half]))
    shells = (shell, frac, pair_shell, pair_frac)
    return backward(
        waves, shells, node_index, node_slope, kernel_table, tables, planes, grid_size
    )


def fits(mesh, length, groups):
    bands, grids = mesh.shape["band"], mesh.shape["grid"]
    planes = length // 2 // bands
    return (
        length == LANES
        and planes == SUBLANES
        and planes % grids == 0
        and planes // grids >= 2
        and bands % 2 == 0
        and bands == SUBLANES
        and (length // grids) % SUBLANES == 0
    )


def solution(mesh):
    placed = (
        P("band", "grid", None, None),
        P("grid", None, None),
        P(None, "grid", None, None),
        P(None, "grid", None, None),
        P(),
    )

    def program(*args):
        length = args[1].shape[0]
        body = per_device
        if fits(mesh, length, args[0].shape[0]):
            bands = mesh.shape["band"]
            tables = constant_tables(length, bands, length // 2 // bands)
            tables = {name: jnp.asarray(table) for name, table in tables.items()}
            body = lambda *blocks: fused_per_device(tables, *blocks)
        return jax.shard_map(
            body, mesh=mesh, in_specs=placed, out_specs=P("grid", None, None), check_vma=False
        )(*args)

    return program
```

```python
import math

import jax
import jax.numpy as jnp
import numpy as np
from jax import lax
from jax.experimental import pallas as pl
from jax.experimental.pallas import tpu as pltpu
from jax.sharding import PartitionSpec as P

def frequency_of(positions, length):
    return jnp.where(positions < length // 2, positions, positions - length)


def shell_split(square_norm):
    root_value = jnp.sqrt(square_norm.astype(jnp.float32))
    shell_idx = root_value.astype(jnp.int32)
    shell_idx = shell_idx - (shell_idx * shell_idx > square_norm).astype(jnp.int32)
    shell_idx = shell_idx + ((shell_idx + 1) * (shell_idx + 1) <= square_norm).astype(jnp.int32)
    fraction = root_value - shell_idx.astype(jnp.float32)
    return (shell_idx, fraction)


def node_fields(count_nodes, intervals, weights):
    node_ids = jnp.arange(count_nodes, dtype=jnp.int32)
    summed = jnp.zeros((count_nodes,) + intervals.shape, jnp.float32)
    for offset in range(4):
        matched = node_ids[:, None, None, None] == (intervals + (offset - 1))[None]
        summed = summed + jnp.where(matched, weights[offset][None], jnp.zeros((), jnp.float32))
    return summed


def phase_table(source_idx, target_idx, modulus):
    product_mod = source_idx[:, None] * target_idx[None, :] % modulus
    angles = product_mod.astype(jnp.float32) * (2.0 * math.pi / modulus)
    return (jnp.cos(angles), jnp.sin(angles))


def contract(pattern, operand, matrix):
    return jnp.einsum(pattern, operand, matrix, precision=lax.Precision.HIGHEST)


def mirrored(values, dim):
    return jnp.roll(jnp.flip(values, dim), 1, dim)


def forward_tables(positions, plane_ids, length):
    cosine, sine = phase_table(positions, plane_ids, length)
    alternating = jnp.where(positions % 2 == 0, 1.0, -1.0).astype(jnp.float32)
    sine = jnp.where(plane_ids[None, :] == 0, -alternating[:, None], sine)
    return (cosine, sine)


def shell_weights_of(square_norm, shell_count):
    shell_ids = jnp.arange(shell_count, dtype=jnp.int32)
    shell_idx, fraction = shell_split(square_norm)
    expand = (slice(None),) + (None,) * square_norm.ndim
    lower_hit = shell_ids[expand] == shell_idx[None]
    upper_hit = shell_ids[expand] == shell_idx[None] + 1
    return jnp.where(lower_hit, 1.0 - fraction[None], 0.0) + jnp.where(
        upper_hit, fraction[None], 0.0
    )


def short(pattern, left, right):
    return jnp.einsum(pattern, left, right, precision=lax.Precision.HIGH)


def halves(values):
    high = values.astype(jnp.bfloat16)
    low = (values - high.astype(jnp.float32)).astype(jnp.bfloat16)
    return high, low


def mix_kernel(count, padded, shell_ref, frac_ref, table_ref, spec_ref, out_ref):
    rows, lanes = shell_ref.shape[1:]
    ids = lax.broadcasted_iota(jnp.int32, (table_ref.shape[1] // 3, lanes), 0)

    def hats(row):
        shell = shell_ref[0, pl.ds(row, 1), :]
        frac = frac_ref[0, pl.ds(row, 1), :]
        return jnp.where(ids == shell, 1.0 - frac, jnp.where(ids == shell + 1, frac, 0.0))

    def step(pair, carry):
        both = jnp.concatenate([hats(2 * pair), hats(2 * pair + 1)], axis=1)
        high, low = halves(both)
        phi = jnp.dot(
            table_ref[...],
            jnp.concatenate([high, high, low], axis=0),
            preferred_element_type=jnp.float32,
        )
        for side in range(2):
            row = 2 * pair + side
            real = jnp.zeros((padded, lanes), jnp.float32)
            imag = jnp.zeros((padded, lanes), jnp.float32)
            for node in range(count):
                part = phi[node * padded : (node + 1) * padded, side * lanes : (side + 1) * lanes]
                real = real + part * spec_ref[0, node, 0, pl.ds(row, 1), :]
                imag = imag + part * spec_ref[1, node, 0, pl.ds(row, 1), :]
            out_ref[0, row, 0] = real[:count]
            out_ref[0, row, 1] = imag[:count]
        return carry

    lax.fori_loop(0, rows // 2, step, 0)


def mix(spectrum, shell, frac, kernel_table):
    _, count, planes, rows, lanes = spectrum.shape
    padded = -(-count // 8) * 8
    depth = -(-(kernel_table.shape[2]) // 128) * 128
    table = jnp.pad(kernel_table, ((0, 0), (0, padded - count), (0, depth - kernel_table.shape[2])))
    table = table.reshape(count * padded, depth)
    rounded = lax.reduce_precision(table, exponent_bits=8, mantissa_bits=7)
    high, low = rounded.astype(jnp.bfloat16), (table - rounded).astype(jnp.bfloat16)
    table = jnp.concatenate([high, low, high], axis=1)
    return pl.pallas_call(
        lambda *refs: mix_kernel(count, padded, *refs),
        grid=(planes,),
        in_specs=[
            pl.BlockSpec((1, rows, lanes), lambda p: (p, 0, 0)),
            pl.BlockSpec((1, rows, lanes), lambda p: (p, 0, 0)),
            pl.BlockSpec(table.shape, lambda p: (0, 0)),
            pl.BlockSpec((2, count, 1, rows, lanes), lambda p: (0, 0, p, 0, 0)),
        ],
        out_specs=pl.BlockSpec((1, rows, 2, count, lanes), lambda p: (p, 0, 0, 0, 0)),
        out_shape=jax.ShapeDtypeStruct((planes, rows, 2, count, lanes), jnp.float32),
    )(shell, frac, table, spectrum)


def per_device(partial_density, node_index, node_weight, node_slope, kernel_table):
    length = node_index.shape[1]
    half = length // 2
    count_nodes = kernel_table.shape[0]
    shell_count = kernel_table.shape[2]
    planes = half // lax.axis_size("band")
    grid_size = lax.axis_size("grid")
    grid_part = length // grid_size
    band_at = lax.axis_index("band")
    grid_at = lax.axis_index("grid")
    full_range = jnp.arange(length, dtype=jnp.int32)
    own_planes = band_at * planes + jnp.arange(planes, dtype=jnp.int32)
    own_rows = grid_at * grid_part + jnp.arange(grid_part, dtype=jnp.int32)
    lower = ((full_range >= 1) & (full_range < half)).astype(jnp.float32)
    upper = (full_range > half).astype(jnp.float32)
    single = 1.0 - lower - upper
    joint = (own_planes == 0)[:, None, None, None, None]
    cosine, sine = phase_table(full_range, full_range, length)
    forward = jnp.stack(
        [jnp.stack([cosine, -sine], 1), jnp.stack([sine, cosine], 1)]
    )
    low_only = lower + single
    packed = jnp.stack(
        [
            jnp.stack([cosine * low_only, -sine * lower], 1),
            jnp.stack([cosine * upper, -sine * upper + cosine * single], 1),
        ]
    )
    forward_y = jnp.where(joint, packed[None], forward[None])
    backward = jnp.stack(
        [jnp.stack([cosine, sine], 1), jnp.stack([-sine, cosine], 1)]
    )
    lower_col, upper_col, single_col = (v[:, None] for v in (lower, upper, single))
    opened = jnp.stack(
        [
            jnp.stack([cosine * (2.0 * lower_col + single_col), cosine * (2.0 * upper_col)], 1),
            jnp.stack(
                [sine * (-2.0 * lower_col), sine * (-2.0 * upper_col) + cosine * single_col], 1
            ),
        ]
    )
    backward_y = jnp.where(joint, opened[None], backward[None])

    density = lax.psum(partial_density[0], "band")
    theta_fields = density[None] * node_fields(count_nodes, node_index, node_weight)
    cosine_z, sine_z = forward_tables(full_range, own_planes, length)
    table_z = jnp.stack([cosine_z, -sine_z], 1)
    columns = short("zcp,axyz->cpaxy", table_z, theta_fields)
    waves = short("cpaxy,pcydw->wdapx", columns, forward_y)
    waves = waves.reshape((grid_size, grid_part) + waves.shape[1:])
    pencils = lax.all_to_all(waves, "grid", split_axis=0, concat_axis=0, tiled=True)
    forward_x = forward.reshape((2, grid_size, grid_part) + forward.shape[2:])
    spectrum = short("gwdapx,dgxev->eapwv", pencils, forward_x)

    freq_x = frequency_of(full_range, length)
    square_x = freq_x * freq_x
    freq_rows = frequency_of(own_rows, length)
    square_rows = freq_rows * freq_rows
    third_square = jnp.where(
        (own_planes[:, None] == 0) & (own_rows[None, :] > half),
        half * half,
        (own_planes * own_planes)[:, None],
    )
    square_norm = (third_square + square_rows[None, :])[:, :, None] + square_x
    shell, frac = shell_split(square_norm)
    mixed = mix(spectrum, shell, frac, kernel_table)

    flag = ((own_rows[0] == 0) | (own_rows[0] == half)) & (own_planes[0] == 0)
    first_norm = square_x + square_rows[0]
    pair_norm = jnp.stack([first_norm, first_norm + half * half])
    kernels = contract("abs,sqx->qabx", kernel_table, shell_weights_of(pair_norm, shell_count))
    spread = (0.5 * flag.astype(jnp.float32)) * (kernels[0] - kernels[1])
    base = spectrum[:, :, 0, 0, :]
    turned = mirrored(base, 2)
    delta = jnp.stack([turned[0] - base[0], -turned[1] - base[1]])
    extra = jnp.sum(spread[None] * delta[:, :, None, :], axis=1)
    mixed = mixed.at[0, 0].add(extra)

    backward_x = backward.reshape(2, length, 2, grid_size, grid_part)
    inverse = short("pwdbv,dvegx->gwebpx", mixed, backward_x)
    returned = lax.all_to_all(inverse, "grid", split_axis=0, concat_axis=0, tiled=True)
    backward_y = backward_y.reshape((planes, 2, grid_size, grid_part, 2, length))
    slab = short("gwdbpx,pdgwcy->cpbxy", returned, backward_y)
    cosine_own, sine_own = phase_table(own_planes, full_range, length)
    alternating = jnp.where(full_range % 2 == 0, 1.0, -1.0).astype(jnp.float32)
    cosine_back = jnp.where(own_planes[:, None] == 0, 1.0, 2.0 * cosine_own)
    sine_back = jnp.where(own_planes[:, None] == 0, -alternating[None, :], 2.0 * sine_own)
    table_back = jnp.stack([cosine_back, -sine_back]) * (1.0 / float(length) ** 3)
    field_parts = short("cpbxy,cpz->bxyz", slab, table_back)
    slopes = node_fields(count_nodes, node_index, node_slope)
    partial_potential = jnp.sum(field_parts * slopes, axis=0)
    return lax.psum(partial_potential, "band")


LANES = 128
SUBLANES = 8
MESH = pl.DeviceIdType.MESH
VMEM = pltpu.VMEM


def split_table(table):
    high = np.asarray(table).astype(jnp.bfloat16)
    low = (np.asarray(table) - high.astype(np.float64)).astype(jnp.bfloat16)
    return high, low


def angles_of(sources, targets, length):
    phase = (np.outer(sources, targets) % length) * (2.0 * np.pi / length)
    return np.cos(phase), np.sin(phase)


def complex_table(cosine, sine):
    return np.stack([np.stack([cosine, -sine], 1), np.stack([sine, cosine], 1)])


def constant_tables(length, bands, planes):
    points = np.arange(length)
    half = length // 2
    cosine, sine = angles_of(points, points, length)
    lower = ((points >= 1) & (points < half)).astype(np.float64)
    upper = (points > half).astype(np.float64)
    single = 1.0 - lower - upper
    forward = complex_table(cosine, sine)
    backward = complex_table(cosine, -sine)
    packed = np.stack(
        [
            np.stack([cosine * (lower + single), -sine * lower], 1),
            np.stack([cosine * upper, -sine * upper + cosine * single], 1),
        ]
    )
    lo, up, one = (v[:, None] for v in (lower, upper, single))
    opened = np.stack(
        [
            np.stack([cosine * (2 * lo + one), cosine * (2 * up)], 1),
            np.stack([sine * (-2 * lo), sine * (-2 * up) + cosine * one], 1),
        ]
    )
    square = (2 * length, 2 * length)

    def right(table):
        high, low = split_table(table.reshape(square))
        return np.concatenate([high, low], 0)

    def left(table):
        high, low = split_table(table.reshape(square).T)
        return np.concatenate([high, low], 1)

    alternating = np.where(points % 2 == 0, 1.0, -1.0)
    z_forward, z_backward = [], []
    for band in range(bands):
        ids = band * planes + np.arange(planes)
        cos_z, sin_z = angles_of(ids, points, length)
        minus = np.where(ids[:, None] == 0, alternating[None], -sin_z)
        rows = np.concatenate([cos_z, minus], 0)
        high, low = split_table(rows)
        top = np.concatenate([high, high], 1)
        bottom = np.concatenate([low, np.zeros_like(low)], 1)
        z_forward.append(np.concatenate([top, bottom], 0))
        first = ids[:, None] == 0
        rows = np.concatenate(
            [np.where(first, 1.0, 2.0 * cos_z), np.where(first, alternating[None], -2.0 * sin_z)]
        ) / float(length) ** 3
        high, low = split_table(rows.T)
        z_backward.append(np.concatenate([high, low, high], 1))
    return {
        "y_forward": np.stack([right(packed), right(forward)]),
        "y_backward": np.stack([right(opened), right(backward)]),
        "x_forward": left(forward),
        "x_backward": left(backward),
        "z_forward": np.stack(z_forward),
        "z_backward": np.stack(z_backward),
    }


def triple_left(values):
    high, low = halves(values)
    return jnp.concatenate([high, low, high], axis=1)


def triple_right(values):
    high, low = halves(values)
    return jnp.concatenate([high, high, low], axis=0)


def right_table(table):
    high, low = table[: table.shape[0] // 2], table[table.shape[0] // 2 :]
    return jnp.concatenate([high, high, low], axis=0)


def left_table(table):
    high, low = table[:, : table.shape[1] // 2], table[:, table.shape[1] // 2 :]
    return jnp.concatenate([high, low, high], axis=1)


def matmul(left, right):
    return jnp.dot(left, right, preferred_element_type=jnp.float32)


def matmul_nt(left, right):
    return lax.dot_general(
        left, right, (((1,), (1,)), ((), ())), preferred_element_type=jnp.float32
    )


def matmul_tn(left, right):
    return lax.dot_general(
        left, right, (((0,), (0,)), ((), ())), preferred_element_type=jnp.float32
    )


def greet(targets):
    barrier = pltpu.get_barrier_semaphore()
    for axis, target in targets:
        pl.semaphore_signal(barrier, inc=1, device_id={axis: target}, device_id_type=MESH)
    pl.semaphore_wait(barrier, len(targets))


class BandSum:
    def __init__(self, outer, chunk_rows, src, dst, near_buf, stage, far_buf, sems):
        me = lax.axis_index("band")
        self.outer, self.src, self.dst = outer, src, dst
        self.near_buf, self.stage, self.far_buf, self.sems = near_buf, stage, far_buf, sems
        self.far, self.near = me // 2, lax.rem(me, 2)
        self.partner = self.far * 2 + (1 - self.near)
        self.others = [lax.rem(self.far + 1 + j, outer) for j in range(outer)]
        self.back = [lax.rem(self.far + outer - 1 - j, outer) for j in range(outer)]
        self.chunk_rows = chunk_rows
        self.side_rows = chunk_rows // 2
        self.part = self.side_rows // outer
        self.peers = [("band", self.partner)] + [
            ("band", o * 2 + self.near) for o in self.others[:-1]
        ]

    def piece(self, chunk, side, quarter):
        start = chunk * self.chunk_rows + side * self.side_rows + quarter * self.part
        return pl.ds(start, self.part)

    def copy(self, src, dst, chunk, kind, j, target):
        return pltpu.make_async_remote_copy(
            src_ref=src,
            dst_ref=dst,
            send_sem=self.sems.at[chunk, kind, 0, j],
            recv_sem=self.sems.at[chunk, kind, 1, j],
            device_id={"band": target},
            device_id_type=MESH,
        )

    def near_copy(self, c, j):
        src = self.src.at[self.piece(c, 1 - self.near, self.others[j])]
        return self.copy(src, self.near_buf.at[c, j], c, 0, j, self.partner)

    def far_copy(self, c, j):
        target = self.others[j] * 2 + self.near
        return self.copy(self.stage.at[c, j], self.far_buf.at[c, j], c, 1, j, target)

    def gather_copy(self, c, j):
        own = self.dst.at[self.piece(c, self.near, self.far)]
        return self.copy(own, own, c, 2, j, self.others[j] * 2 + self.near)

    def pass_copy(self, c, j):
        block = self.dst.at[self.piece(c, self.near, self.back[j])]
        return self.copy(block, block, c, 3, j, self.partner)

    def start(self, c):
        for j in range(self.outer):
            self.near_copy(c, j).start()

    def reduce(self, c):
        for j in range(self.outer - 1):
            self.near_copy(c, j).wait_recv()
            mine = self.src[self.piece(c, self.near, self.others[j])]
            self.stage[c, j] = mine + self.near_buf[c, j]
            self.far_copy(c, j).start()

    def finish(self, c):
        last = self.outer - 1
        self.near_copy(c, last).wait_recv()
        own = self.piece(c, self.near, self.far)
        total = self.src[own] + self.near_buf[c, last]
        for j in range(last):
            self.far_copy(c, j).wait_recv()
            total = total + self.far_buf[c, j]
        self.dst[own] = total
        for j in range(last):
            self.gather_copy(c, j).start()
        self.pass_copy(c, last).start()

    def forward(self, c):
        for j in range(self.outer - 1):
            self.gather_copy(c, j).wait_recv()
            self.pass_copy(c, j).start()

    def arrive(self, c):
        for j in range(self.outer):
            self.pass_copy(c, j).wait_recv()

    def drain(self, c):
        for j in range(self.outer):
            self.near_copy(c, j).wait_send()
            self.pass_copy(c, j).wait_send()
        for j in range(self.outer - 1):
            self.far_copy(c, j).wait_send()
            self.gather_copy(c, j).wait_send()


def whole_kernel(
    sizes,
    partial_hbm,
    index_hbm,
    weight_hbm,
    slope_hbm,
    table_ref,
    tz_ref,
    ty_ref,
    tx_ref,
    ti_ref,
    bz_ref,
    by_ref,
    out_ref,
    density_ref,
    index_ref,
    weight_ref,
    theta,
    columns,
    ahead,
    waves,
    shells,
    fracs,
    spec,
    mixed,
    phi,
    delta,
    extra,
    home,
    back,
    slab,
    turned,
    ids_ref,
    fields,
    total_ref,
    ahead_sems,
    home_sems,
    load_sems,
    near_buf,
    stage,
    far_buf,
    density_sems,
    potential_sems,
):
    count, padded, grid_size, planes, length, outer = sizes
    per = planes // grid_size
    grid_part = length // grid_size
    steps = grid_part // SUBLANES
    early = steps - 1
    rows = count * SUBLANES
    pitch = rows + SUBLANES
    half = length // 2
    pairs = half // 2 + 1
    wide = 2 * length
    band_at, me = lax.axis_index("band"), lax.axis_index("grid")
    order = [lax.rem(me + 1 + j, grid_size) for j in range(grid_size)]
    remote = range(grid_size - 1)
    joint = (band_at == 0) & (me == 0)
    buffers = (near_buf, stage, far_buf)
    summed = BandSum(outer, SUBLANES, out_ref, density_ref, *buffers, density_sems)
    result = BandSum(outer, SUBLANES, density_ref, out_ref, *buffers, potential_sems)

    partial_load = pltpu.make_async_copy(partial_hbm, out_ref, load_sems.at[0])
    index_load = pltpu.make_async_copy(index_hbm, index_ref, load_sems.at[1])
    weight_load = pltpu.make_async_copy(weight_hbm, weight_ref, load_sems.at[2])
    slope_load = pltpu.make_async_copy(slope_hbm, weight_ref, load_sems.at[3])
    partial_load.start()
    greet(summed.peers + [("grid", target) for target in order[:-1]])
    partial_load.wait()
    summed.start(0)
    index_load.start()
    weight_load.start()

    def norms():
        lane = lax.broadcasted_iota(jnp.int32, shells.shape[1:], 1)
        row = lax.broadcasted_iota(jnp.int32, shells.shape[1:], 0)
        side = (lane >= length).astype(jnp.int32)
        ky = lane - side * length
        fx, fy = frequency_of(2 * row + side, length), frequency_of(ky, length)
        for k in range(per):
            kz = band_at * planes + me * per + k
            folded = jnp.where(ky > half, half * half, 0)
            third = jnp.where(kz == 0, folded, kz * kz)
            shells[k], fracs[k] = shell_split(fx * fx + fy * fy + third)
        once = fy * fy + side * half * half
        shells[per], fracs[per] = shell_split(once + row * half * half)

    def ahead_copy(step, j, k):
        return pltpu.make_async_remote_copy(
            src_ref=ahead.at[step, j, k],
            dst_ref=waves.at[k, :, me * steps + step],
            send_sem=ahead_sems.at[0, step, j, k],
            recv_sem=ahead_sems.at[1, step, j, k],
            device_id={"grid": order[j]},
            device_id_type=MESH,
        )

    def home_copy(step, j, k):
        return pltpu.make_async_remote_copy(
            src_ref=home.at[order[j], step, k],
            dst_ref=back.at[step, me, k],
            send_sem=home_sems.at[0, step, j, k],
            recv_sem=home_sems.at[1, step, j, k],
            device_id={"grid": order[j]},
            device_id_type=MESH,
        )

    def own_copy(step):
        sem = home_sems.at[0, step, grid_size - 1, 0]
        return pltpu.make_async_copy(home.at[me, step], back.at[step, me], sem)

    block = 32
    half_rows = SUBLANES // 2

    def fill(step, part):
        def body(at, carry):
            x_at = step * SUBLANES + part * half_rows + at // (length // block)
            start = pl.multiple_of(lax.rem(at, length // block) * block, block)
            place = pl.ds(pl.multiple_of(at * block, block), block)
            index = index_ref[x_at, pl.ds(start, block), :] - 1
            amount = density_ref[x_at, pl.ds(start, block), :]
            parts = [amount * weight_ref[j, x_at, pl.ds(start, block), :] for j in range(4)]
            for node in range(count):
                value = jnp.where(index == node, parts[0], 0.0)
                for j in range(1, 4):
                    value = jnp.where(index == node - j, parts[j], value)
                high, low = halves(value)
                theta[node, place, 0:length] = high
                theta[node, place, length:wide] = low
            return carry

        lax.fori_loop(0, half_rows * length // block, body, 0)

    def columns_of(part):
        table = tz_ref[band_at]

        def body(node, carry):
            for pair in range(half_rows // 2):
                out = matmul_nt(table, theta[node, pair * wide : (pair + 1) * wide, :])
                out = out[: 2 * planes] + out[2 * planes :]
                for side in range(2):
                    for c in range(2):
                        row = c * planes * pitch + node * SUBLANES + part * half_rows
                        columns[pl.ds(row + pair * 2 + side, planes, stride=pitch), :] = out[
                            c * planes : (c + 1) * planes, side * length : (side + 1) * length
                        ]
            return carry

        lax.fori_loop(0, count, body, 0)

    def waves_of(step, j, k):
        plane = order[j] * per + k
        start = pl.multiple_of(plane * pitch, SUBLANES)
        left = jnp.concatenate(
            [columns[pl.ds(c * planes * pitch + start, rows), :] for c in range(2)], axis=1
        )
        kind = jnp.minimum(plane + band_at * planes, 1)
        out = matmul(triple_left(left), right_table(ty_ref[kind]))
        for d in range(2):
            value = out[:, d * length : (d + 1) * length]
            if j < grid_size - 1:
                ahead[step, j, k, d] = value
            else:
                waves[k, d, me * steps + step] = value

    def advance(call, chunk):
        if chunk < steps:
            call(chunk)

    norms()
    advance(summed.start, 1)
    summed.reduce(0)
    summed.finish(0)
    advance(summed.reduce, 1)
    summed.forward(0)
    advance(summed.start, 2)
    index_load.wait()
    weight_load.wait()
    for step in range(steps):
        summed.arrive(step)
        fill(step, 0)
        columns_of(0)
        advance(summed.finish, step + 1)
        advance(summed.reduce, step + 2)
        fill(step, 1)
        columns_of(1)
        advance(summed.forward, step + 1)
        advance(summed.start, step + 3)
        for k in range(per):
            for j in range(grid_size):
                waves_of(step, j, k)
                if j < grid_size - 1 and (step < early or k < per - 1):
                    ahead_copy(step, j, k).start()
    for step in range(early, steps):
        for j in remote:
            ahead_copy(step, j, per - 1).start()
    slope_load.start()
    for step in range(steps):
        summed.drain(step)

    lane = lax.broadcasted_iota(jnp.int32, (16, length), 1)
    slot = lax.broadcasted_iota(jnp.int32, (16, length), 0)
    chosen = jnp.where((lane == slot * half) & (slot < 2), 1.0, 0.0).astype(jnp.bfloat16)
    ids = lax.broadcasted_iota(jnp.int32, (table_ref.shape[1] // 3, wide), 0)

    def hats(k, row):
        shell, frac = shells[k, pl.ds(row, 1), :], fracs[k, pl.ds(row, 1), :]
        return jnp.where(ids == shell, 1.0 - frac, jnp.where(ids == shell + 1, frac, 0.0))

    def points_of(node, k, d):
        start = node * SUBLANES
        if not isinstance(node, int):
            start = pl.multiple_of(start, SUBLANES)
        return waves[k, d, :, pl.ds(start, SUBLANES), :].reshape(length, length)

    def mix_rows(choices, load):
        sums = [
            [jnp.zeros((padded, length), jnp.float32) for _ in range(4)] for _ in range(choices)
        ]
        for node in range(count):
            for tile in range(2):
                part = phi[node * padded : (node + 1) * padded, tile * length : (tile + 1) * length]
                for choice in range(choices):
                    for e in range(2):
                        value = part * load(node, e, choice, tile)
                        sums[choice][2 * e + tile] = sums[choice][2 * e + tile] + value
        return sums

    def correction():
        right = jnp.concatenate(
            [tx_ref[:, length:wide], tx_ref[:, wide + length : 2 * wide]], axis=1
        )

        lines = []
        for node in range(count):
            high, low = halves(points_of(node, 0, 1))
            lines.append((matmul_nt(chosen, high) + matmul_nt(chosen, low))[:SUBLANES])
        high, low = halves(-2.0 * jnp.concatenate(lines, axis=0))
        both = jnp.concatenate([high, high], axis=1)
        out = matmul_nt(both, right)
        low = jnp.concatenate([low, jnp.zeros_like(low)], axis=1)
        out = out + matmul_nt(low, right)
        delta[...] = out.reshape(count, SUBLANES, wide)
        phi[...] = matmul(table_ref[...], triple_right(0.5 * (hats(per, 0) - hats(per, 1))))
        sums = mix_rows(
            1,
            lambda node, e, choice, tile: delta[
                node, tile : tile + 1, e * length : (e + 1) * length
            ],
        )[0]
        inverse = jnp.concatenate(
            [ti_ref[:, 0:wide], ti_ref[:, 0:wide], ti_ref[:, wide : 2 * wide]], axis=1
        )
        for r in range(2):
            left = jnp.concatenate([sums[r], sums[2 + r]], axis=1)
            added = matmul_nt(triple_left(left), inverse)
            for c in range(2):
                value = added[:, c * length : (c + 1) * length]
                extra[c, pl.ds(r, padded, stride=SUBLANES), :] = value

    def middle(k):
        for step in range(steps):
            for j in remote:
                ahead_copy(step, j, k).wait_recv()

        def to_spectrum(pair, carry):
            values = jnp.concatenate(
                [
                    jnp.concatenate([points_of(2 * pair + side, k, d) for side in range(2)], axis=1)
                    for d in range(2)
                ],
                axis=0,
            )
            out = matmul(left_table(tx_ref[...]), triple_right(values))
            for side in range(2):
                spec[2 * pair + side] = out[:, side * length : (side + 1) * length]
            return carry

        lax.fori_loop(0, count // 2, to_spectrum, 0)

        def mix_pair(t, carry):
            phi[...] = matmul(table_ref[...], triple_right(hats(k, t)))
            at = [[2 * t, 2 * t + 1]]
            at.append([lax.rem(length - i, length) for i in at[0]])
            sums = mix_rows(
                2,
                lambda node, e, choice, tile: spec[
                    node, pl.ds(e * length + at[choice][tile], 1), :
                ],
            )
            for choice in range(2):
                for e in range(2):
                    for tile in range(2):
                        start = (e * length + at[choice][tile]) * padded
                        place = pl.ds(pl.multiple_of(start, SUBLANES), padded)
                        mixed[place, :] = sums[choice][2 * e + tile]
            return carry

        lax.fori_loop(0, pairs, mix_pair, 0)
        if k == 0:
            extra[...] = jnp.zeros_like(extra)
            pl.when(joint)(correction)

        def to_slabs(pair, carry):
            nodes = [2 * pair + side for side in range(2)]
            lines = [mixed[pl.ds(node, wide, stride=padded), :] for node in nodes]
            out = matmul(left_table(ti_ref[...]), triple_right(jnp.concatenate(lines, axis=1)))
            for side, node in enumerate(nodes):
                place = pl.ds(pl.multiple_of(node * SUBLANES, SUBLANES), SUBLANES)
                value = out[:, side * length : (side + 1) * length]
                if k == 0:
                    line = jnp.concatenate([extra[c, place, :] for c in range(2)], axis=1)
                    both = jnp.concatenate(halves(line), axis=0)
                    mask = jnp.concatenate([chosen[:SUBLANES], chosen[:SUBLANES]], axis=0)
                    value = value + matmul_tn(both, mask)
                for c in range(2):
                    part = value[c * length : (c + 1) * length]
                    part = part.reshape(grid_size, steps, SUBLANES, length)
                    home[:, :, k, c, place, :] = part
            return carry

        lax.fori_loop(0, count // 2, to_slabs, 0)

    for k in range(per):
        middle(k)
        for step in range(early):
            for j in remote:
                home_copy(step, j, k).start()
    for step in range(early, steps):
        for k in range(per):
            for j in remote:
                home_copy(step, j, k).start()
    for step in range(steps):
        own_copy(step).start()
    slope_load.wait()
    table = bz_ref[band_at]

    def y_rows(step):
        def body(plane, carry):
            kind = jnp.minimum(plane + band_at * planes, 1)
            left = jnp.concatenate(
                [back[step, plane // per, lax.rem(plane, per), c] for c in range(2)], axis=1
            )
            out = matmul(triple_left(left), right_table(by_ref[kind]))
            for c in range(2):
                start = pl.multiple_of((c * planes + plane) * pitch, SUBLANES)
                slab[pl.ds(start, rows), :] = out[:, c * length : (c + 1) * length]
            return carry

        lax.fori_loop(0, planes, body, 0)

    def z_rows(step):
        def pair_of(pair, carry):
            first = step * SUBLANES + pair * 2
            for side in range(2):
                lanes = slice(side * length, (side + 1) * length)
                ids_ref[:, lanes] = index_ref[first + side].T - 1
                for j in range(4):
                    turned[j, :, lanes] = weight_ref[j, first + side].T
            for node in range(count):
                sides = []
                for side in range(2):
                    start = node * SUBLANES + pair * 2 + side
                    parts = [
                        slab[pl.ds(c * planes * pitch + start, planes, stride=pitch), :]
                        for c in range(2)
                    ]
                    sides.append(jnp.concatenate(parts, axis=0))
                fields[node] = matmul(table, triple_right(jnp.concatenate(sides, axis=1)))

            def pick(block, carry):
                place = pl.ds(pl.multiple_of(block * SUBLANES, SUBLANES), SUBLANES)
                index = ids_ref[place, :]
                picked = [jnp.zeros((SUBLANES, wide), jnp.float32) for _ in range(4)]
                for node in range(count):
                    field = fields[node, place, :]
                    for j in range(4):
                        picked[j] = jnp.where(index == node - j, field, picked[j])
                summed = picked[0] * turned[0, place, :]
                for j in range(1, 4):
                    summed = summed + picked[j] * turned[j, place, :]
                total_ref[place, :] = summed
                return carry

            lax.fori_loop(0, length // SUBLANES, pick, 0)
            for side in range(2):
                lanes = slice(side * length, (side + 1) * length)
                density_ref[first + side] = total_ref[:, lanes].T
            return carry

        lax.fori_loop(0, SUBLANES // 2, pair_of, 0)

    for at in range(steps):
        own_copy(at).wait()
        for j in remote:
            for k in range(per):
                home_copy(at, j, k).wait_recv()
        y_rows(at)
        z_rows(at)
        result.start(at)
        if at > 0:
            result.finish(at - 1)
        result.reduce(at)
        if at > 0:
            result.forward(at - 1)
    result.finish(steps - 1)
    result.forward(steps - 1)
    for step in range(steps):
        result.arrive(step)
        result.drain(step)
        for j in remote:
            for k in range(per):
                ahead_copy(step, j, k).wait_send()
                home_copy(step, j, k).wait_send()


def fused_per_device(tables, partial_density, node_index, node_weight, node_slope, kernel_table):
    grid_part, length = node_index.shape[:2]
    count = kernel_table.shape[0]
    planes = length // 2 // lax.axis_size("band")
    grid_size = lax.axis_size("grid")
    outer = lax.axis_size("band") // 2
    per = planes // grid_size
    steps = grid_part // SUBLANES
    rows = count * SUBLANES
    wide = 2 * length
    padded = -(-count // SUBLANES) * SUBLANES
    depth = -(-(kernel_table.shape[2]) // LANES) * LANES
    table = jnp.pad(kernel_table, ((0, 0), (0, padded - count), (0, depth - kernel_table.shape[2])))
    table = table.reshape(count * padded, depth)
    rounded = lax.reduce_precision(table, exponent_bits=8, mantissa_bits=7)
    high, low = rounded.astype(jnp.bfloat16), (table - rounded).astype(jnp.bfloat16)
    table = jnp.concatenate([high, low, high], axis=1)
    sizes = (count, padded, grid_size, planes, length, outer)
    pairs = -(-(length // 4 + 1) // SUBLANES) * SUBLANES
    piece = (SUBLANES // (2 * outer), length, length)
    floats = lambda *shape: VMEM(shape, jnp.float32)
    dma = lambda *shape: pltpu.SemaphoreType.DMA(shape)
    whole = pl.BlockSpec(memory_space=VMEM)
    anywhere = pl.BlockSpec(memory_space=pl.ANY)
    return pl.pallas_call(
        lambda *refs: whole_kernel(sizes, *refs),
        in_specs=[anywhere] * 4 + [whole] * 7,
        out_specs=whole,
        out_shape=jax.ShapeDtypeStruct(node_index.shape, jnp.float32),
        scratch_shapes=[
            floats(*node_index.shape),
            VMEM(node_index.shape, jnp.int32),
            floats(*node_weight.shape),
            VMEM((count, SUBLANES // 2 * length, wide), jnp.bfloat16),
            floats(2 * planes * (rows + SUBLANES), length),
            floats(steps, grid_size - 1, per, 2, rows, length),
            floats(per, 2, grid_size * steps, rows, length),
            VMEM((per + 1, pairs, wide), jnp.int32),
            floats(per + 1, pairs, wide),
            floats(count, wide, length),
            floats(wide * padded, length),
            floats(count * padded, wide),
            floats(count, SUBLANES, wide),
            floats(2, padded * SUBLANES, length),
            floats(grid_size, steps, per, 2, rows, length),
            floats(steps, grid_size, per, 2, rows, length),
            floats(2 * planes * (rows + SUBLANES), length),
            floats(4, length, wide),
            VMEM((length, wide), jnp.int32),
            floats(count, length, wide),
            floats(length, wide),
            dma(2, steps, grid_size - 1, per),
            dma(2, steps, grid_size, per),
            dma(4),
            floats(steps, outer, *piece),
            floats(steps, outer - 1, *piece),
            floats(steps, outer - 1, *piece),
            dma(steps, 4, 2, outer),
            dma(steps, 4, 2, outer),
        ],
        compiler_params=pltpu.CompilerParams(
            collective_id=1, has_side_effects=True, vmem_limit_bytes=67043328
        ),
    )(
        partial_density[0],
        node_index,
        node_weight,
        node_slope,
        table,
        tables["z_forward"],
        tables["y_forward"],
        tables["x_forward"],
        tables["x_backward"],
        tables["z_backward"],
        tables["y_backward"],
    )


def fits(mesh, length, count):
    bands, grids = mesh.shape["band"], mesh.shape["grid"]
    planes = length // 2 // bands
    return (
        length == LANES
        and planes == SUBLANES
        and planes % grids == 0
        and planes // grids >= 2
        and bands % 2 == 0
        and bands == SUBLANES
        and count % 2 == 0
        and (length // grids) % SUBLANES == 0
    )


def solution(mesh):
    placed = (
        P("band", "grid", None, None),
        P("grid", None, None),
        P(None, "grid", None, None),
        P(None, "grid", None, None),
        P(),
    )

    def program(*args):
        length = args[1].shape[0]
        body = per_device
        if fits(mesh, length, args[4].shape[0]):
            bands = mesh.shape["band"]
            tables = constant_tables(length, bands, length // 2 // bands)
            tables = {name: jnp.asarray(table) for name, table in tables.items()}
            body = lambda *blocks: fused_per_device(tables, *blocks)
        return jax.shard_map(
            body, mesh=mesh, in_specs=placed, out_specs=P("grid", None, None), check_vma=False
        )(*args)

    return program
```

```python
import math

import jax
import jax.numpy as jnp
import numpy as np
from jax import lax
from jax.experimental import pallas as pl
from jax.experimental.pallas import tpu as pltpu
from jax.sharding import PartitionSpec as P

def frequency_of(positions, length):
    return jnp.where(positions < length // 2, positions, positions - length)


def shell_split(square_norm):
    root_value = jnp.sqrt(square_norm.astype(jnp.float32))
    shell_idx = root_value.astype(jnp.int32)
    shell_idx = shell_idx - (shell_idx * shell_idx > square_norm).astype(jnp.int32)
    shell_idx = shell_idx + ((shell_idx + 1) * (shell_idx + 1) <= square_norm).astype(jnp.int32)
    fraction = root_value - shell_idx.astype(jnp.float32)
    return (shell_idx, fraction)


def node_fields(count_nodes, intervals, weights):
    node_ids = jnp.arange(count_nodes, dtype=jnp.int32)
    summed = jnp.zeros((count_nodes,) + intervals.shape, jnp.float32)
    for offset in range(4):
        matched = node_ids[:, None, None, None] == (intervals + (offset - 1))[None]
        summed = summed + jnp.where(matched, weights[offset][None], jnp.zeros((), jnp.float32))
    return summed


def phase_table(source_idx, target_idx, modulus):
    product_mod = source_idx[:, None] * target_idx[None, :] % modulus
    angles = product_mod.astype(jnp.float32) * (2.0 * math.pi / modulus)
    return (jnp.cos(angles), jnp.sin(angles))


def contract(pattern, operand, matrix):
    return jnp.einsum(pattern, operand, matrix, precision=lax.Precision.HIGHEST)


def mirrored(values, dim):
    return jnp.roll(jnp.flip(values, dim), 1, dim)


def forward_tables(positions, plane_ids, length):
    cosine, sine = phase_table(positions, plane_ids, length)
    alternating = jnp.where(positions % 2 == 0, 1.0, -1.0).astype(jnp.float32)
    sine = jnp.where(plane_ids[None, :] == 0, -alternating[:, None], sine)
    return (cosine, sine)


def shell_weights_of(square_norm, shell_count):
    shell_ids = jnp.arange(shell_count, dtype=jnp.int32)
    shell_idx, fraction = shell_split(square_norm)
    expand = (slice(None),) + (None,) * square_norm.ndim
    lower_hit = shell_ids[expand] == shell_idx[None]
    upper_hit = shell_ids[expand] == shell_idx[None] + 1
    return jnp.where(lower_hit, 1.0 - fraction[None], 0.0) + jnp.where(
        upper_hit, fraction[None], 0.0
    )


def short(pattern, left, right):
    return jnp.einsum(pattern, left, right, precision=lax.Precision.HIGH)


def halves(values):
    high = values.astype(jnp.bfloat16)
    low = (values - high.astype(jnp.float32)).astype(jnp.bfloat16)
    return high, low


def mix_kernel(count, padded, shell_ref, frac_ref, table_ref, spec_ref, out_ref):
    rows, lanes = shell_ref.shape[1:]
    ids = lax.broadcasted_iota(jnp.int32, (table_ref.shape[1] // 3, lanes), 0)

    def hats(row):
        shell = shell_ref[0, pl.ds(row, 1), :]
        frac = frac_ref[0, pl.ds(row, 1), :]
        return jnp.where(ids == shell, 1.0 - frac, jnp.where(ids == shell + 1, frac, 0.0))

    def step(pair, carry):
        both = jnp.concatenate([hats(2 * pair), hats(2 * pair + 1)], axis=1)
        high, low = halves(both)
        phi = jnp.dot(
            table_ref[...],
            jnp.concatenate([high, high, low], axis=0),
            preferred_element_type=jnp.float32,
        )
        for side in range(2):
            row = 2 * pair + side
            real = jnp.zeros((padded, lanes), jnp.float32)
            imag = jnp.zeros((padded, lanes), jnp.float32)
            for node in range(count):
                part = phi[node * padded : (node + 1) * padded, side * lanes : (side + 1) * lanes]
                real = real + part * spec_ref[0, node, 0, pl.ds(row, 1), :]
                imag = imag + part * spec_ref[1, node, 0, pl.ds(row, 1), :]
            out_ref[0, row, 0] = real[:count]
            out_ref[0, row, 1] = imag[:count]
        return carry

    lax.fori_loop(0, rows // 2, step, 0)


def mix(spectrum, shell, frac, kernel_table):
    _, count, planes, rows, lanes = spectrum.shape
    padded = -(-count // 8) * 8
    depth = -(-(kernel_table.shape[2]) // 128) * 128
    table = jnp.pad(kernel_table, ((0, 0), (0, padded - count), (0, depth - kernel_table.shape[2])))
    table = table.reshape(count * padded, depth)
    rounded = lax.reduce_precision(table, exponent_bits=8, mantissa_bits=7)
    high, low = rounded.astype(jnp.bfloat16), (table - rounded).astype(jnp.bfloat16)
    table = jnp.concatenate([high, low, high], axis=1)
    return pl.pallas_call(
        lambda *refs: mix_kernel(count, padded, *refs),
        grid=(planes,),
        in_specs=[
            pl.BlockSpec((1, rows, lanes), lambda p: (p, 0, 0)),
            pl.BlockSpec((1, rows, lanes), lambda p: (p, 0, 0)),
            pl.BlockSpec(table.shape, lambda p: (0, 0)),
            pl.BlockSpec((2, count, 1, rows, lanes), lambda p: (0, 0, p, 0, 0)),
        ],
        out_specs=pl.BlockSpec((1, rows, 2, count, lanes), lambda p: (p, 0, 0, 0, 0)),
        out_shape=jax.ShapeDtypeStruct((planes, rows, 2, count, lanes), jnp.float32),
    )(shell, frac, table, spectrum)


def per_device(partial_density, node_index, node_weight, node_slope, kernel_table):
    length = node_index.shape[1]
    half = length // 2
    count_nodes = kernel_table.shape[0]
    shell_count = kernel_table.shape[2]
    planes = half // lax.axis_size("band")
    grid_size = lax.axis_size("grid")
    grid_part = length // grid_size
    band_at = lax.axis_index("band")
    grid_at = lax.axis_index("grid")
    full_range = jnp.arange(length, dtype=jnp.int32)
    own_planes = band_at * planes + jnp.arange(planes, dtype=jnp.int32)
    own_rows = grid_at * grid_part + jnp.arange(grid_part, dtype=jnp.int32)
    lower = ((full_range >= 1) & (full_range < half)).astype(jnp.float32)
    upper = (full_range > half).astype(jnp.float32)
    single = 1.0 - lower - upper
    joint = (own_planes == 0)[:, None, None, None, None]
    cosine, sine = phase_table(full_range, full_range, length)
    forward = jnp.stack(
        [jnp.stack([cosine, -sine], 1), jnp.stack([sine, cosine], 1)]
    )
    low_only = lower + single
    packed = jnp.stack(
        [
            jnp.stack([cosine * low_only, -sine * lower], 1),
            jnp.stack([cosine * upper, -sine * upper + cosine * single], 1),
        ]
    )
    forward_y = jnp.where(joint, packed[None], forward[None])
    backward = jnp.stack(
        [jnp.stack([cosine, sine], 1), jnp.stack([-sine, cosine], 1)]
    )
    lower_col, upper_col, single_col = (v[:, None] for v in (lower, upper, single))
    opened = jnp.stack(
        [
            jnp.stack([cosine * (2.0 * lower_col + single_col), cosine * (2.0 * upper_col)], 1),
            jnp.stack(
                [sine * (-2.0 * lower_col), sine * (-2.0 * upper_col) + cosine * single_col], 1
            ),
        ]
    )
    backward_y = jnp.where(joint, opened[None], backward[None])

    density = lax.psum(partial_density[0], "band")
    theta_fields = density[None] * node_fields(count_nodes, node_index, node_weight)
    cosine_z, sine_z = forward_tables(full_range, own_planes, length)
    table_z = jnp.stack([cosine_z, -sine_z], 1)
    columns = short("zcp,axyz->cpaxy", table_z, theta_fields)
    waves = short("cpaxy,pcydw->wdapx", columns, forward_y)
    waves = waves.reshape((grid_size, grid_part) + waves.shape[1:])
    pencils = lax.all_to_all(waves, "grid", split_axis=0, concat_axis=0, tiled=True)
    forward_x = forward.reshape((2, grid_size, grid_part) + forward.shape[2:])
    spectrum = short("gwdapx,dgxev->eapwv", pencils, forward_x)

    freq_x = frequency_of(full_range, length)
    square_x = freq_x * freq_x
    freq_rows = frequency_of(own_rows, length)
    square_rows = freq_rows * freq_rows
    third_square = jnp.where(
        (own_planes[:, None] == 0) & (own_rows[None, :] > half),
        half * half,
        (own_planes * own_planes)[:, None],
    )
    square_norm = (third_square + square_rows[None, :])[:, :, None] + square_x
    shell, frac = shell_split(square_norm)
    mixed = mix(spectrum, shell, frac, kernel_table)

    flag = ((own_rows[0] == 0) | (own_rows[0] == half)) & (own_planes[0] == 0)
    first_norm = square_x + square_rows[0]
    pair_norm = jnp.stack([first_norm, first_norm + half * half])
    kernels = contract("abs,sqx->qabx", kernel_table, shell_weights_of(pair_norm, shell_count))
    spread = (0.5 * flag.astype(jnp.float32)) * (kernels[0] - kernels[1])
    base = spectrum[:, :, 0, 0, :]
    turned = mirrored(base, 2)
    delta = jnp.stack([turned[0] - base[0], -turned[1] - base[1]])
    extra = jnp.sum(spread[None] * delta[:, :, None, :], axis=1)
    mixed = mixed.at[0, 0].add(extra)

    backward_x = backward.reshape(2, length, 2, grid_size, grid_part)
    inverse = short("pwdbv,dvegx->gwebpx", mixed, backward_x)
    returned = lax.all_to_all(inverse, "grid", split_axis=0, concat_axis=0, tiled=True)
    backward_y = backward_y.reshape((planes, 2, grid_size, grid_part, 2, length))
    slab = short("gwdbpx,pdgwcy->cpbxy", returned, backward_y)
    cosine_own, sine_own = phase_table(own_planes, full_range, length)
    alternating = jnp.where(full_range % 2 == 0, 1.0, -1.0).astype(jnp.float32)
    cosine_back = jnp.where(own_planes[:, None] == 0, 1.0, 2.0 * cosine_own)
    sine_back = jnp.where(own_planes[:, None] == 0, -alternating[None, :], 2.0 * sine_own)
    table_back = jnp.stack([cosine_back, -sine_back]) * (1.0 / float(length) ** 3)
    field_parts = short("cpbxy,cpz->bxyz", slab, table_back)
    slopes = node_fields(count_nodes, node_index, node_slope)
    partial_potential = jnp.sum(field_parts * slopes, axis=0)
    return lax.psum(partial_potential, "band")


LANES = 128
SUBLANES = 8
MESH = pl.DeviceIdType.MESH
VMEM = pltpu.VMEM


def split_table(table):
    high = np.asarray(table).astype(jnp.bfloat16)
    low = (np.asarray(table) - high.astype(np.float64)).astype(jnp.bfloat16)
    return high, low


def angles_of(sources, targets, length):
    phase = (np.outer(sources, targets) % length) * (2.0 * np.pi / length)
    return np.cos(phase), np.sin(phase)


def complex_table(cosine, sine):
    return np.stack([np.stack([cosine, -sine], 1), np.stack([sine, cosine], 1)])


def constant_tables(length, bands, planes):
    points = np.arange(length)
    half = length // 2
    cosine, sine = angles_of(points, points, length)
    lower = ((points >= 1) & (points < half)).astype(np.float64)
    upper = (points > half).astype(np.float64)
    single = 1.0 - lower - upper
    forward = complex_table(cosine, sine)
    backward = complex_table(cosine, -sine)
    packed = np.stack(
        [
            np.stack([cosine * (lower + single), -sine * lower], 1),
            np.stack([cosine * upper, -sine * upper + cosine * single], 1),
        ]
    )
    lo, up, one = (v[:, None] for v in (lower, upper, single))
    opened = np.stack(
        [
            np.stack([cosine * (2 * lo + one), cosine * (2 * up)], 1),
            np.stack([sine * (-2 * lo), sine * (-2 * up) + cosine * one], 1),
        ]
    )
    square = (2 * length, 2 * length)

    def right(table):
        high, low = split_table(table.reshape(square))
        return np.concatenate([high, low], 0)

    def left(table):
        high, low = split_table(table.reshape(square).T)
        return np.concatenate([high, low], 1)

    alternating = np.where(points % 2 == 0, 1.0, -1.0)
    z_forward, z_backward = [], []
    for band in range(bands):
        ids = band * planes + np.arange(planes)
        cos_z, sin_z = angles_of(ids, points, length)
        minus = np.where(ids[:, None] == 0, alternating[None], -sin_z)
        rows = np.concatenate([cos_z, minus], 0)
        high, low = split_table(rows)
        top = np.concatenate([high, high], 1)
        bottom = np.concatenate([low, np.zeros_like(low)], 1)
        z_forward.append(np.concatenate([top, bottom], 0))
        first = ids[:, None] == 0
        rows = np.concatenate(
            [np.where(first, 1.0, 2.0 * cos_z), np.where(first, alternating[None], -2.0 * sin_z)]
        ) / float(length) ** 3
        high, low = split_table(rows.T)
        z_backward.append(np.concatenate([high, low, high], 1))
    return {
        "y_forward": np.stack([right(packed), right(forward)]),
        "y_backward": np.stack([right(opened), right(backward)]),
        "x_forward": left(forward),
        "x_backward": left(backward),
        "z_forward": np.stack(z_forward),
        "z_backward": np.stack(z_backward),
    }


def triple_left(values):
    high, low = halves(values)
    return jnp.concatenate([high, low, high], axis=1)


def triple_right(values):
    high, low = halves(values)
    return jnp.concatenate([high, high, low], axis=0)


def right_table(table):
    high, low = table[: table.shape[0] // 2], table[table.shape[0] // 2 :]
    return jnp.concatenate([high, high, low], axis=0)


def left_table(table):
    high, low = table[:, : table.shape[1] // 2], table[:, table.shape[1] // 2 :]
    return jnp.concatenate([high, low, high], axis=1)


def matmul(left, right):
    return jnp.dot(left, right, preferred_element_type=jnp.float32)


def matmul_nt(left, right):
    return lax.dot_general(
        left, right, (((1,), (1,)), ((), ())), preferred_element_type=jnp.float32
    )


def matmul_tn(left, right):
    return lax.dot_general(
        left, right, (((0,), (0,)), ((), ())), preferred_element_type=jnp.float32
    )


def greet(targets):
    barrier = pltpu.get_barrier_semaphore()
    for axis, target in targets:
        pl.semaphore_signal(barrier, inc=1, device_id={axis: target}, device_id_type=MESH)
    pl.semaphore_wait(barrier, len(targets))


class BandSum:
    def __init__(self, outer, chunk_rows, src, dst, near_buf, stage, far_buf, sems):
        me = lax.axis_index("band")
        self.outer, self.src, self.dst = outer, src, dst
        self.near_buf, self.stage, self.far_buf, self.sems = near_buf, stage, far_buf, sems
        self.far, self.near = me // 2, lax.rem(me, 2)
        self.partner = self.far * 2 + (1 - self.near)
        self.others = [lax.rem(self.far + 1 + j, outer) for j in range(outer)]
        self.back = [lax.rem(self.far + outer - 1 - j, outer) for j in range(outer)]
        self.chunk_rows = chunk_rows
        self.side_rows = chunk_rows // 2
        self.part = self.side_rows // outer
        self.peers = [("band", self.partner)] + [
            ("band", o * 2 + self.near) for o in self.others[:-1]
        ]

    def piece(self, chunk, side, quarter):
        start = chunk * self.chunk_rows + side * self.side_rows + quarter * self.part
        return pl.ds(start, self.part)

    def copy(self, src, dst, chunk, kind, j, target):
        return pltpu.make_async_remote_copy(
            src_ref=src,
            dst_ref=dst,
            send_sem=self.sems.at[chunk, kind, 0, j],
            recv_sem=self.sems.at[chunk, kind, 1, j],
            device_id={"band": target},
            device_id_type=MESH,
        )

    def near_copy(self, c, j):
        src = self.src.at[self.piece(c, 1 - self.near, self.others[j])]
        return self.copy(src, self.near_buf.at[c, j], c, 0, j, self.partner)

    def far_copy(self, c, j):
        target = self.others[j] * 2 + self.near
        return self.copy(self.stage.at[c, j], self.far_buf.at[c, j], c, 1, j, target)

    def gather_copy(self, c, j):
        own = self.dst.at[self.piece(c, self.near, self.far)]
        return self.copy(own, own, c, 2, j, self.others[j] * 2 + self.near)

    def pass_copy(self, c, j):
        block = self.dst.at[self.piece(c, self.near, self.back[j])]
        return self.copy(block, block, c, 3, j, self.partner)

    def start(self, c):
        for j in range(self.outer):
            self.near_copy(c, j).start()

    def reduce(self, c):
        for j in range(self.outer - 1):
            self.near_copy(c, j).wait_recv()
            mine = self.src[self.piece(c, self.near, self.others[j])]
            self.stage[c, j] = mine + self.near_buf[c, j]
            self.far_copy(c, j).start()

    def finish(self, c):
        last = self.outer - 1
        self.near_copy(c, last).wait_recv()
        own = self.piece(c, self.near, self.far)
        total = self.src[own] + self.near_buf[c, last]
        for j in range(last):
            self.far_copy(c, j).wait_recv()
            total = total + self.far_buf[c, j]
        self.dst[own] = total
        for j in range(last):
            self.gather_copy(c, j).start()
        self.pass_copy(c, last).start()

    def forward(self, c):
        for j in range(self.outer - 1):
            self.gather_copy(c, j).wait_recv()
            self.pass_copy(c, j).start()

    def arrive(self, c):
        for j in range(self.outer):
            self.pass_copy(c, j).wait_recv()

    def drain(self, c):
        for j in range(self.outer):
            self.near_copy(c, j).wait_send()
            self.pass_copy(c, j).wait_send()
        for j in range(self.outer - 1):
            self.far_copy(c, j).wait_send()
            self.gather_copy(c, j).wait_send()


def whole_kernel(
    sizes,
    partial_hbm,
    index_hbm,
    weight_hbm,
    slope_hbm,
    table_ref,
    tz_ref,
    ty_ref,
    tx_ref,
    ti_ref,
    bz_ref,
    by_ref,
    out_ref,
    density_ref,
    index_ref,
    weight_ref,
    theta,
    columns,
    ahead,
    waves,
    shells,
    fracs,
    spec,
    mixed,
    phi,
    other,
    delta,
    extra,
    home,
    back,
    slab,
    turned,
    ids_ref,
    fields,
    total_ref,
    ahead_sems,
    home_sems,
    load_sems,
    near_buf,
    stage,
    far_buf,
    density_sems,
    potential_sems,
):
    count, padded, grid_size, planes, length, outer = sizes
    per = planes // grid_size
    grid_part = length // grid_size
    steps = grid_part // SUBLANES
    early = steps - 1
    rows = count * SUBLANES
    pitch = rows + SUBLANES
    half = length // 2
    pairs = half // 2 + 1
    wide = 2 * length
    band_at, me = lax.axis_index("band"), lax.axis_index("grid")
    order = [lax.rem(me + 1 + j, grid_size) for j in range(grid_size)]
    remote = range(grid_size - 1)
    joint = (band_at == 0) & (me == 0)
    buffers = (near_buf, stage, far_buf)
    summed = BandSum(outer, SUBLANES, out_ref, density_ref, *buffers, density_sems)
    result = BandSum(outer, SUBLANES, density_ref, out_ref, *buffers, potential_sems)

    partial_load = pltpu.make_async_copy(partial_hbm, out_ref, load_sems.at[0])
    index_load = pltpu.make_async_copy(index_hbm, index_ref, load_sems.at[1])
    weight_load = pltpu.make_async_copy(weight_hbm, weight_ref, load_sems.at[2])
    slope_load = pltpu.make_async_copy(slope_hbm, weight_ref, load_sems.at[3])
    partial_load.start()
    greet(summed.peers + [("grid", target) for target in order[:-1]])
    partial_load.wait()
    summed.start(0)
    index_load.start()
    weight_load.start()

    def norms():
        lane = lax.broadcasted_iota(jnp.int32, shells.shape[1:], 1)
        row = lax.broadcasted_iota(jnp.int32, shells.shape[1:], 0)
        side = (lane >= length).astype(jnp.int32)
        ky = lane - side * length
        fx, fy = frequency_of(2 * row + side, length), frequency_of(ky, length)
        for k in range(per):
            kz = band_at * planes + me * per + k
            folded = jnp.where(ky > half, half * half, 0)
            third = jnp.where(kz == 0, folded, kz * kz)
            shells[k], fracs[k] = shell_split(fx * fx + fy * fy + third)
        once = fy * fy + side * half * half
        shells[per], fracs[per] = shell_split(once + row * half * half)

    def ahead_copy(step, j, k):
        return pltpu.make_async_remote_copy(
            src_ref=ahead.at[step, j, k],
            dst_ref=waves.at[k, :, me * steps + step],
            send_sem=ahead_sems.at[0, step, j, k],
            recv_sem=ahead_sems.at[1, step, j, k],
            device_id={"grid": order[j]},
            device_id_type=MESH,
        )

    def home_copy(step, j, k):
        return pltpu.make_async_remote_copy(
            src_ref=home.at[order[j], step, k],
            dst_ref=back.at[step, me, k],
            send_sem=home_sems.at[0, step, j, k],
            recv_sem=home_sems.at[1, step, j, k],
            device_id={"grid": order[j]},
            device_id_type=MESH,
        )

    def own_copy(step):
        sem = home_sems.at[0, step, grid_size - 1, 0]
        return pltpu.make_async_copy(home.at[me, step], back.at[step, me], sem)

    block = 32
    half_rows = SUBLANES // 2

    def fill(step, part):
        def body(at, carry):
            x_at = step * SUBLANES + part * half_rows + at // (length // block)
            start = pl.multiple_of(lax.rem(at, length // block) * block, block)
            place = pl.ds(pl.multiple_of(at * block, block), block)
            index = index_ref[x_at, pl.ds(start, block), :] - 1
            amount = density_ref[x_at, pl.ds(start, block), :]
            parts = [amount * weight_ref[j, x_at, pl.ds(start, block), :] for j in range(4)]
            for node in range(count):
                value = jnp.where(index == node, parts[0], 0.0)
                for j in range(1, 4):
                    value = jnp.where(index == node - j, parts[j], value)
                high, low = halves(value)
                theta[node, place, 0:length] = high
                theta[node, place, length:wide] = low
            return carry

        lax.fori_loop(0, half_rows * length // block, body, 0)

    def columns_of(part):
        table = tz_ref[band_at]

        def body(node, carry):
            for pair in range(half_rows // 2):
                out = matmul_nt(table, theta[node, pair * wide : (pair + 1) * wide, :])
                out = out[: 2 * planes] + out[2 * planes :]
                for side in range(2):
                    for c in range(2):
                        row = c * planes * pitch + node * SUBLANES + part * half_rows
                        columns[pl.ds(row + pair * 2 + side, planes, stride=pitch), :] = out[
                            c * planes : (c + 1) * planes, side * length : (side + 1) * length
                        ]
            return carry

        lax.fori_loop(0, count, body, 0)

    def waves_of(step, j, k):
        plane = order[j] * per + k
        start = pl.multiple_of(plane * pitch, SUBLANES)
        left = jnp.concatenate(
            [columns[pl.ds(c * planes * pitch + start, rows), :] for c in range(2)], axis=1
        )
        kind = jnp.minimum(plane + band_at * planes, 1)
        out = matmul(triple_left(left), right_table(ty_ref[kind]))
        for d in range(2):
            value = out[:, d * length : (d + 1) * length]
            if j < grid_size - 1:
                ahead[step, j, k, d] = value
            else:
                waves[k, d, me * steps + step] = value

    def advance(call, chunk):
        if chunk < steps:
            call(chunk)

    norms()
    advance(summed.start, 1)
    summed.reduce(0)
    summed.finish(0)
    advance(summed.reduce, 1)
    summed.forward(0)
    advance(summed.start, 2)
    index_load.wait()
    weight_load.wait()
    for step in range(steps):
        summed.arrive(step)
        advance(summed.finish, step + 1)
        fill(step, 0)
        columns_of(0)
        advance(summed.reduce, step + 2)
        advance(summed.forward, step + 1)
        fill(step, 1)
        columns_of(1)
        advance(summed.start, step + 3)
        for k in range(per):
            for j in range(grid_size):
                waves_of(step, j, k)
                if j < grid_size - 1 and (step < early or k < per - 1):
                    ahead_copy(step, j, k).start()
    for step in range(early, steps):
        for j in remote:
            ahead_copy(step, j, per - 1).start()
    slope_load.start()
    for step in range(steps):
        summed.drain(step)

    lane = lax.broadcasted_iota(jnp.int32, (16, length), 1)
    slot = lax.broadcasted_iota(jnp.int32, (16, length), 0)
    chosen = jnp.where((lane == slot * half) & (slot < 2), 1.0, 0.0).astype(jnp.bfloat16)
    ids = lax.broadcasted_iota(jnp.int32, (table_ref.shape[1] // 3, wide), 0)

    def hats(k, row):
        shell, frac = shells[k, pl.ds(row, 1), :], fracs[k, pl.ds(row, 1), :]
        return jnp.where(ids == shell, 1.0 - frac, jnp.where(ids == shell + 1, frac, 0.0))

    def points_of(node, k, d):
        start = node * SUBLANES
        if not isinstance(node, int):
            start = pl.multiple_of(start, SUBLANES)
        return waves[k, d, :, pl.ds(start, SUBLANES), :].reshape(length, length)

    def mix_rows(phi, choices, load):
        sums = [
            [jnp.zeros((padded, length), jnp.float32) for _ in range(4)] for _ in range(choices)
        ]
        for node in range(count):
            for tile in range(2):
                part = phi[node * padded : (node + 1) * padded, tile * length : (tile + 1) * length]
                for choice in range(choices):
                    for e in range(2):
                        value = part * load(node, e, choice, tile)
                        sums[choice][2 * e + tile] = sums[choice][2 * e + tile] + value
        return sums

    def correction():
        right = jnp.concatenate(
            [tx_ref[:, length:wide], tx_ref[:, wide + length : 2 * wide]], axis=1
        )

        lines = []
        for node in range(count):
            high, low = halves(points_of(node, 0, 1))
            lines.append((matmul_nt(chosen, high) + matmul_nt(chosen, low))[:SUBLANES])
        high, low = halves(-2.0 * jnp.concatenate(lines, axis=0))
        both = jnp.concatenate([high, high], axis=1)
        out = matmul_nt(both, right)
        low = jnp.concatenate([low, jnp.zeros_like(low)], axis=1)
        out = out + matmul_nt(low, right)
        delta[...] = out.reshape(count, SUBLANES, wide)
        phi[...] = matmul(table_ref[...], triple_right(0.5 * (hats(per, 0) - hats(per, 1))))
        sums = mix_rows(
            phi,
            1,
            lambda node, e, choice, tile: delta[
                node, tile : tile + 1, e * length : (e + 1) * length
            ],
        )[0]
        inverse = jnp.concatenate(
            [ti_ref[:, 0:wide], ti_ref[:, 0:wide], ti_ref[:, wide : 2 * wide]], axis=1
        )
        for r in range(2):
            left = jnp.concatenate([sums[r], sums[2 + r]], axis=1)
            added = matmul_nt(triple_left(left), inverse)
            for c in range(2):
                value = added[:, c * length : (c + 1) * length]
                extra[c, pl.ds(r, padded, stride=SUBLANES), :] = value

    def middle(k):
        for step in range(steps):
            for j in remote:
                ahead_copy(step, j, k).wait_recv()

        def to_spectrum(pair, carry):
            values = jnp.concatenate(
                [
                    jnp.concatenate([points_of(2 * pair + side, k, d) for side in range(2)], axis=1)
                    for d in range(2)
                ],
                axis=0,
            )
            out = matmul(left_table(tx_ref[...]), triple_right(values))
            for side in range(2):
                spec[2 * pair + side] = out[:, side * length : (side + 1) * length]
            return carry

        lax.fori_loop(0, count // 2, to_spectrum, 0)

        def mix_pair(phi, t):
            at = [[2 * t, 2 * t + 1]]
            at.append([lax.rem(length - i, length) for i in at[0]])
            sums = mix_rows(
                phi,
                2,
                lambda node, e, choice, tile: spec[
                    node, pl.ds(e * length + at[choice][tile], 1), :
                ],
            )
            for choice in range(2):
                for e in range(2):
                    for tile in range(2):
                        start = (e * length + at[choice][tile]) * padded
                        place = pl.ds(pl.multiple_of(start, SUBLANES), padded)
                        mixed[place, :] = sums[choice][2 * e + tile]

        def weigh(target, t):
            target[...] = matmul(table_ref[...], triple_right(hats(k, t)))

        def mix_two(i, carry):
            weigh(other, 2 * i + 1)
            mix_pair(phi, 2 * i)
            weigh(phi, 2 * i + 2)
            mix_pair(other, 2 * i + 1)
            return carry

        weigh(phi, 0)
        lax.fori_loop(0, pairs // 2, mix_two, 0)
        mix_pair(phi, pairs - 1)
        if k == 0:
            extra[...] = jnp.zeros_like(extra)
            pl.when(joint)(correction)

        def to_slabs(pair, carry):
            nodes = [2 * pair + side for side in range(2)]
            lines = [mixed[pl.ds(node, wide, stride=padded), :] for node in nodes]
            out = matmul(left_table(ti_ref[...]), triple_right(jnp.concatenate(lines, axis=1)))
            for side, node in enumerate(nodes):
                place = pl.ds(pl.multiple_of(node * SUBLANES, SUBLANES), SUBLANES)
                value = out[:, side * length : (side + 1) * length]
                if k == 0:
                    line = jnp.concatenate([extra[c, place, :] for c in range(2)], axis=1)
                    both = jnp.concatenate(halves(line), axis=0)
                    mask = jnp.concatenate([chosen[:SUBLANES], chosen[:SUBLANES]], axis=0)
                    value = value + matmul_tn(both, mask)
                for c in range(2):
                    part = value[c * length : (c + 1) * length]
                    part = part.reshape(grid_size, steps, SUBLANES, length)
                    home[:, :, k, c, place, :] = part
            return carry

        lax.fori_loop(0, count // 2, to_slabs, 0)

    for k in range(per):
        middle(k)
        for step in range(early):
            for j in remote:
                home_copy(step, j, k).start()
    for step in range(early, steps):
        for k in range(per):
            for j in remote:
                home_copy(step, j, k).start()
    for step in range(steps):
        own_copy(step).start()
    slope_load.wait()
    table = bz_ref[band_at]

    def y_rows(step):
        def body(plane, carry):
            kind = jnp.minimum(plane + band_at * planes, 1)
            left = jnp.concatenate(
                [back[step, plane // per, lax.rem(plane, per), c] for c in range(2)], axis=1
            )
            out = matmul(triple_left(left), right_table(by_ref[kind]))
            for c in range(2):
                start = pl.multiple_of((c * planes + plane) * pitch, SUBLANES)
                slab[pl.ds(start, rows), :] = out[:, c * length : (c + 1) * length]
            return carry

        lax.fori_loop(0, planes, body, 0)

    def z_rows(step):
        def pair_of(pair, carry):
            first = step * SUBLANES + pair * 2
            for side in range(2):
                lanes = slice(side * length, (side + 1) * length)
                ids_ref[:, lanes] = index_ref[first + side].T - 1
                for j in range(4):
                    turned[j, :, lanes] = weight_ref[j, first + side].T
            for node in range(count):
                sides = []
                for side in range(2):
                    start = node * SUBLANES + pair * 2 + side
                    parts = [
                        slab[pl.ds(c * planes * pitch + start, planes, stride=pitch), :]
                        for c in range(2)
                    ]
                    sides.append(jnp.concatenate(parts, axis=0))
                fields[node] = matmul(table, triple_right(jnp.concatenate(sides, axis=1)))

            def pick(block, carry):
                place = pl.ds(pl.multiple_of(block * SUBLANES, SUBLANES), SUBLANES)
                index = ids_ref[place, :]
                picked = [jnp.zeros((SUBLANES, wide), jnp.float32) for _ in range(4)]
                for node in range(count):
                    field = fields[node, place, :]
                    for j in range(4):
                        picked[j] = jnp.where(index == node - j, field, picked[j])
                summed = picked[0] * turned[0, place, :]
                for j in range(1, 4):
                    summed = summed + picked[j] * turned[j, place, :]
                total_ref[place, :] = summed
                return carry

            lax.fori_loop(0, length // SUBLANES, pick, 0)
            for side in range(2):
                lanes = slice(side * length, (side + 1) * length)
                density_ref[first + side] = total_ref[:, lanes].T
            return carry

        lax.fori_loop(0, SUBLANES // 2, pair_of, 0)

    for at in range(steps):
        own_copy(at).wait()
        for j in remote:
            for k in range(per):
                home_copy(at, j, k).wait_recv()
        y_rows(at)
        z_rows(at)
        result.start(at)
        if at > 0:
            result.finish(at - 1)
        result.reduce(at)
        if at > 0:
            result.forward(at - 1)
    result.finish(steps - 1)
    result.forward(steps - 1)
    for step in range(steps):
        result.arrive(step)
        result.drain(step)
        for j in remote:
            for k in range(per):
                ahead_copy(step, j, k).wait_send()
                home_copy(step, j, k).wait_send()


def fused_per_device(tables, partial_density, node_index, node_weight, node_slope, kernel_table):
    grid_part, length = node_index.shape[:2]
    count = kernel_table.shape[0]
    planes = length // 2 // lax.axis_size("band")
    grid_size = lax.axis_size("grid")
    outer = lax.axis_size("band") // 2
    per = planes // grid_size
    steps = grid_part // SUBLANES
    rows = count * SUBLANES
    wide = 2 * length
    padded = -(-count // SUBLANES) * SUBLANES
    depth = -(-(kernel_table.shape[2]) // LANES) * LANES
    table = jnp.pad(kernel_table, ((0, 0), (0, padded - count), (0, depth - kernel_table.shape[2])))
    table = table.reshape(count * padded, depth)
    rounded = lax.reduce_precision(table, exponent_bits=8, mantissa_bits=7)
    high, low = rounded.astype(jnp.bfloat16), (table - rounded).astype(jnp.bfloat16)
    table = jnp.concatenate([high, low, high], axis=1)
    sizes = (count, padded, grid_size, planes, length, outer)
    pairs = -(-(length // 4 + 1) // SUBLANES) * SUBLANES
    piece = (SUBLANES // (2 * outer), length, length)
    floats = lambda *shape: VMEM(shape, jnp.float32)
    dma = lambda *shape: pltpu.SemaphoreType.DMA(shape)
    whole = pl.BlockSpec(memory_space=VMEM)
    anywhere = pl.BlockSpec(memory_space=pl.ANY)
    return pl.pallas_call(
        lambda *refs: whole_kernel(sizes, *refs),
        in_specs=[anywhere] * 4 + [whole] * 7,
        out_specs=whole,
        out_shape=jax.ShapeDtypeStruct(node_index.shape, jnp.float32),
        scratch_shapes=[
            floats(*node_index.shape),
            VMEM(node_index.shape, jnp.int32),
            floats(*node_weight.shape),
            VMEM((count, SUBLANES // 2 * length, wide), jnp.bfloat16),
            floats(2 * planes * (rows + SUBLANES), length),
            floats(steps, grid_size - 1, per, 2, rows, length),
            floats(per, 2, grid_size * steps, rows, length),
            VMEM((per + 1, pairs, wide), jnp.int32),
            floats(per + 1, pairs, wide),
            floats(count, wide, length),
            floats(wide * padded, length),
            floats(count * padded, wide),
            floats(count * padded, wide),
            floats(count, SUBLANES, wide),
            floats(2, padded * SUBLANES, length),
            floats(grid_size, steps, per, 2, rows, length),
            floats(steps, grid_size, per, 2, rows, length),
            floats(2 * planes * (rows + SUBLANES), length),
            floats(4, length, wide),
            VMEM((length, wide), jnp.int32),
            floats(count, length, wide),
            floats(length, wide),
            dma(2, steps, grid_size - 1, per),
            dma(2, steps, grid_size, per),
            dma(4),
            floats(steps, outer, *piece),
            floats(steps, outer - 1, *piece),
            floats(steps, outer - 1, *piece),
            dma(steps, 4, 2, outer),
            dma(steps, 4, 2, outer),
        ],
        compiler_params=pltpu.CompilerParams(
            collective_id=1, has_side_effects=True, vmem_limit_bytes=67043328
        ),
    )(
        partial_density[0],
        node_index,
        node_weight,
        node_slope,
        table,
        tables["z_forward"],
        tables["y_forward"],
        tables["x_forward"],
        tables["x_backward"],
        tables["z_backward"],
        tables["y_backward"],
    )


def fits(mesh, length, count):
    bands, grids = mesh.shape["band"], mesh.shape["grid"]
    planes = length // 2 // bands
    return (
        length == LANES
        and planes == SUBLANES
        and planes % grids == 0
        and planes // grids >= 2
        and bands % 2 == 0
        and bands == SUBLANES
        and count % 2 == 0
        and (length // 4) % 2 == 0
        and (length // grids) % SUBLANES == 0
    )


def solution(mesh):
    placed = (
        P("band", "grid", None, None),
        P("grid", None, None),
        P(None, "grid", None, None),
        P(None, "grid", None, None),
        P(),
    )

    def program(*args):
        length = args[1].shape[0]
        body = per_device
        if fits(mesh, length, args[4].shape[0]):
            bands = mesh.shape["band"]
            tables = constant_tables(length, bands, length // 2 // bands)
            tables = {name: jnp.asarray(table) for name, table in tables.items()}
            body = lambda *blocks: fused_per_device(tables, *blocks)
        return jax.shard_map(
            body, mesh=mesh, in_specs=placed, out_specs=P("grid", None, None), check_vma=False
        )(*args)

    return program
```
